8 devices in a mesh: dp: 1 (over z), vp: 2 (over y), tp: 4 (over x, core).
Axes of the slice: x: 2, y: 2, z: 1, core: 2. Of those that a mesh axis runs over, the one named last changes fastest.
Arguments:
- hidden: bfloat16 [16, 1024], P('dp', 'tp')
- lnf_gain: float32 [1024], P('tp')
- lnf_bias: float32 [1024], P('tp')
- emb_table: bfloat16 [250880, 1024], P('vp', 'tp')
- next_tok: int32 [16], P('dp')
- eln_gain: float32 [1024], P('tp')
- eln_bias: float32 [1024], P('tp')
Outputs:
- output 1: float32 [16, 250880], P('dp', ('vp', 'tp'))
- output 2: float32 [16], P('dp')
- output 3: bfloat16 [16, 1024], P('dp', 'tp')
All inputs are finite; a program needn't handle non-finite values.
Results may differ from the reference program's by a relative error of at most 0.001.
Values sent between devices are 32-bit elements.
A program may use at most 1 GiB of HBM per device.

```python
import jax
import jax.numpy as jnp

BATCH_ROWS = 16
D = 1024
VOCAB_SIZE = 250880
VP_BLOCKS = 2
HOT_COUNT = min(2, VP_BLOCKS)
NORM_EPS = 1e-5


def draw_tokens(key):
    key_hot, key_pick, key_any, key_sel, key_pos = jax.random.split(key, 5)
    block_len = VOCAB_SIZE // VP_BLOCKS
    hot_blocks = jax.random.permutation(key_hot, VP_BLOCKS)[:HOT_COUNT]
    hot_pick = jax.random.randint(key_pick, (BATCH_ROWS,), 0, HOT_COUNT)
    any_block = jax.random.randint(key_any, (BATCH_ROWS,), 0, VP_BLOCKS)
    use_hot = jax.random.randint(key_sel, (BATCH_ROWS,), 0, 4) < 3
    tok_block = jnp.where(use_hot, hot_blocks[hot_pick], any_block)
    tok_within = jax.random.randint(key_pos, (BATCH_ROWS,), 0, block_len)
    return (tok_block * block_len + tok_within).astype(jnp.int32)


def setup_inputs(seed: int = 0, part: int = 0) -> dict:
    shared_key, part_root = jax.random.split(jax.random.key(seed))
    part_key = jax.random.fold_in(part_root, part)
    key_hid, key_off, key_tok = jax.random.split(part_key, 3)
    key_tab, key_rowm, key_g1, key_b1, key_g2, key_b2 = jax.random.split(shared_key, 6)
    col_pos = jnp.arange(D, dtype=jnp.float32) / D
    hidden = jax.random.normal(key_hid, (BATCH_ROWS, D), jnp.float32) * (0.5 + 1.5 * col_pos)
    hidden = hidden + jax.random.normal(key_off, (BATCH_ROWS, 1), jnp.float32) * (1.0 + 2.0 * col_pos)
    tab_vals = jax.random.normal(key_tab, (VOCAB_SIZE, D), jnp.float32) * (0.5 + col_pos)
    tab_vals = (tab_vals + jax.random.normal(key_rowm, (VOCAB_SIZE, 1), jnp.float32)) * (D ** -0.5)
    return {
        "hidden": hidden.astype(jnp.bfloat16),
        "lnf_gain": 1.5 + 0.5 * jax.random.normal(key_g1, (D,), jnp.float32),
        "lnf_bias": 0.5 * jax.random.normal(key_b1, (D,), jnp.float32),
        "emb_table": tab_vals.astype(jnp.bfloat16),
        "next_tok": draw_tokens(key_tok),
        "eln_gain": 1.0 + 0.3 * jax.random.normal(key_g2, (D,), jnp.float32),
        "eln_bias": 0.5 * jax.random.normal(key_b2, (D,), jnp.float32),
    }


def layer_norm(rows_in, norm_gain, norm_bias):
    rows_f32 = rows_in.astype(jnp.float32)
    row_mean = jnp.mean(rows_f32, axis=-1, keepdims=True)
    row_var = jnp.mean(rows_f32 * rows_f32, axis=-1, keepdims=True) - row_mean * row_mean
    return (rows_f32 - row_mean) / jnp.sqrt(row_var + NORM_EPS) * norm_gain + norm_bias


def reference(hidden, lnf_gain, lnf_bias, emb_table, next_tok, eln_gain, eln_bias):
    normed = layer_norm(hidden, lnf_gain, lnf_bias).astype(jnp.bfloat16)
    logits = jnp.dot(normed, emb_table.T, preferred_element_type=jnp.float32)
    log_sum = jax.nn.logsumexp(logits, axis=-1)
    logprobs = logits - log_sum[:, None]
    tok_rows = jnp.take(emb_table, next_tok, axis=0)
    next_in = layer_norm(tok_rows, eln_gain, eln_bias).astype(jnp.bfloat16)
    return (logprobs, log_sum, next_in)
```

```python
import functools

import jax
import jax.numpy as jnp
from jax import lax
from jax.experimental import pallas as pl
from jax.experimental.pallas import tpu as pltpu
from jax.sharding import PartitionSpec as P

NORM_EPS = 1e-5
MESH = pl.DeviceIdType.MESH
LANES = 128
SLOTS = 4
LAG = 3


def chunk_of(block):
    tiles = block // LANES
    return LANES * max(d for d in range(1, 9) if tiles % d == 0)


def pack_sums(rows_f32):
    sums = jnp.sum(rows_f32, axis=1, keepdims=True)
    squares = jnp.sum(rows_f32 * rows_f32, axis=1, keepdims=True)
    shape = (rows_f32.shape[0], LANES)
    lane = lax.broadcasted_iota(jnp.int32, shape, 1)
    return jnp.where(lane < LANES // 2, jnp.broadcast_to(sums, shape), jnp.broadcast_to(squares, shape))


def apply_norm(rows_f32, packed, gain, bias, full_width):
    half = LANES // 2
    mean = packed[:, 0:1] / full_width
    var = packed[:, half : half + 1] / full_width - mean * mean
    scaled = (rows_f32 - mean) * lax.rsqrt(var + NORM_EPS)
    return (scaled * gain + bias).astype(jnp.bfloat16)


def main_kernel(
    vp_size, chunk, n_chunks, full_width,
    hid_ref, g1_ref, b1_ref, table_ref, pick_ref, g2_ref, b2_ref,
    z_ref, ls_ref, nxt_ref,
    tab, xn, mine, give, take, land, st, row_in, es, fs,
    tab_sem, give_sem, take_sem, push_sem, land_sem,
    st_ssem, st_rsem, row_ssem, row_rsem, es_ssem, es_rsem, fs_ssem, fs_rsem,
):
    v = lax.axis_index("vp")
    t = lax.axis_index("tp")
    n_dev = vp_size * 4
    me = v * 4 + t
    core = t % 2
    chip = t // 2
    sib = chip * 2 + 1 - core
    across = (1 - chip) * 2 + core
    diag = (1 - chip) * 2 + 1 - core
    block = chunk * n_chunks
    n_steps = 2 * n_chunks

    def table_copy(step, part):
        far = 1 - step // n_chunks
        owner_chip = chip + far - 2 * chip * far
        owner_core = core + (1 - part) - 2 * core * (1 - part)
        start = (owner_chip * 2 + owner_core) * block + (step % n_chunks) * chunk
        slot = step % SLOTS
        return pltpu.make_async_copy(
            table_ref.at[pl.ds(pl.multiple_of(start, LANES), chunk), :],
            tab.at[slot, part],
            tab_sem.at[slot, part],
        )

    for s in range(SLOTS):
        table_copy(s, 0).start()
        table_copy(s, 1).start()

    barrier = pltpu.get_barrier_semaphore()
    for d in range(1, n_dev):
        other = (me + d) % n_dev
        pl.semaphore_signal(barrier, inc=1, device_id={"vp": other // 4, "tp": other % 4}, device_id_type=MESH)

    hid = hid_ref[...].astype(jnp.float32)
    st[t] = pack_sums(hid)
    pl.semaphore_wait(barrier, n_dev - 1)

    stat_copies = []
    for i, target in enumerate((across, diag, sib)):
        copy = pltpu.make_async_remote_copy(
            st.at[t], st.at[t], st_ssem.at[i], st_rsem.at[i], device_id={"tp": target}, device_id_type=MESH
        )
        copy.start()
        stat_copies.append(copy)
    row_copies = []
    for d in range(1, vp_size):
        copy = pltpu.make_async_remote_copy(
            pick_ref, row_in.at[d - 1], row_ssem.at[d - 1], row_rsem.at[d - 1],
            device_id={"vp": (v + d) % vp_size}, device_id_type=MESH,
        )
        copy.start()
        row_copies.append(copy)
    for copy in stat_copies:
        copy.wait_recv()
    total = st[0] + st[1] + st[2] + st[3]
    xn[...] = apply_norm(hid, total, g1_ref[...], b1_ref[...], full_width)

    def give_copy(step):
        return pltpu.make_async_remote_copy(
            give.at[step], take.at[step], give_sem.at[step], take_sem.at[step],
            device_id={"tp": sib}, device_id_type=MESH,
        )

    def push_copy(j):
        return pltpu.make_async_remote_copy(
            mine.at[j], land.at[j], push_sem.at[j], land_sem.at[j],
            device_id={"tp": across}, device_id_type=MESH,
        )

    def dot_part(slot, part):
        return lax.dot_general(
            xn[...], tab[slot, part], (((1,), (1,)), ((), ())), preferred_element_type=jnp.float32
        )

    def combine(step):
        give_copy(step).wait_recv()
        mine[step] = mine[step] + take[step]

    def produce(step):
        slot = step % SLOTS
        table_copy(step, 0).wait()
        give[step] = dot_part(slot, 0)
        give_copy(step).start()
        table_copy(step, 1).wait()
        mine[step] = dot_part(slot, 1)

        @pl.when(step + SLOTS < n_steps)
        def _():
            table_copy(step + SLOTS, 0).start()
            table_copy(step + SLOTS, 1).start()

    def far_step(step, carry):
        produce(step)

        @pl.when(step >= LAG)
        def _():
            combine(step - LAG)
            push_copy(step - LAG).start()

        return carry

    lax.fori_loop(0, n_chunks, far_step, 0)
    for j in range(n_chunks - LAG, n_chunks):
        combine(j)
        push_copy(j).start()

    rows = pick_ref[...]
    for d in range(1, vp_size):
        row_copies[d - 1].wait_recv()
        rows = rows + row_in[d - 1]
    es[t] = pack_sums(rows)
    sum_copies = []
    for i, target in enumerate((across, diag, sib)):
        copy = pltpu.make_async_remote_copy(
            es.at[t], es.at[t], es_ssem.at[i], es_rsem.at[i], device_id={"tp": target}, device_id_type=MESH
        )
        copy.start()
        sum_copies.append(copy)

    def near_step(step, carry):
        produce(step)

        @pl.when(step >= n_chunks + LAG)
        def _():
            combine(step - LAG)

        return carry

    lax.fori_loop(n_chunks, n_steps, near_step, 0)
    for j in range(n_steps - LAG, n_steps):
        combine(j)

    for copy in sum_copies:
        copy.wait_recv()
    row_total = es[0] + es[1] + es[2] + es[3]
    nxt_ref[...] = apply_norm(rows, row_total, g2_ref[...], b2_ref[...], full_width)

    n_rows = hid.shape[0]

    def finish(j, carry):
        top, acc = carry
        push_copy(j).wait_recv()
        vals = mine[n_chunks + j] + land[j]
        z_ref[:, pl.ds(pl.multiple_of(j * chunk, LANES), chunk)] = vals
        tiles = [vals[:, i * LANES : (i + 1) * LANES] for i in range(chunk // LANES)]
        new_top = functools.reduce(jnp.maximum, tiles, top)
        acc = acc * jnp.exp(top - new_top)
        for tile in tiles:
            acc = acc + jnp.exp(tile - new_top)
        return new_top, acc

    top, acc = lax.fori_loop(
        0, n_chunks, finish,
        (jnp.full((n_rows, LANES), -jnp.inf, jnp.float32), jnp.zeros((n_rows, LANES), jnp.float32)),
    )
    row_top = jnp.max(top, axis=1, keepdims=True)
    row_sum = jnp.sum(acc * jnp.exp(top - row_top), axis=1, keepdims=True)
    lane = lax.broadcasted_iota(jnp.int32, (n_rows, LANES), 1)
    fs[me] = jnp.where(
        lane < LANES // 2, jnp.broadcast_to(row_top, (n_rows, LANES)), jnp.broadcast_to(row_sum, (n_rows, LANES))
    )
    last_copies = []
    for d in range(1, n_dev):
        other = (me + d) % n_dev
        copy = pltpu.make_async_remote_copy(
            fs.at[me], fs.at[me], fs_ssem.at[d - 1], fs_rsem.at[d - 1],
            device_id={"vp": other // 4, "tp": other % 4}, device_id_type=MESH,
        )
        copy.start()
        last_copies.append(copy)
    for copy in last_copies:
        copy.wait_recv()
    half = LANES // 2
    all_top = functools.reduce(jnp.maximum, [fs[i][:, 0:half] for i in range(n_dev)])
    all_sum = jnp.zeros_like(all_top)
    for i in range(n_dev):
        all_sum = all_sum + fs[i][:, half:] * jnp.exp(fs[i][:, 0:half] - all_top)
    ls_ref[...] = all_top + jnp.log(all_sum)

    for copy in stat_copies + row_copies + sum_copies + last_copies:
        copy.wait_send()

    def drain(step, carry):
        give_copy(step).wait_send()
        return carry

    lax.fori_loop(0, n_steps, drain, 0)

    def drain_push(j, carry):
        push_copy(j).wait_send()
        return carry

    lax.fori_loop(0, n_chunks, drain_push, 0)


def solution(mesh):
    tp_size = mesh.shape["tp"]
    vp_size = mesh.shape["vp"]

    def per_device(hidden, lnf_gain, lnf_bias, emb_table, next_tok, eln_gain, eln_bias):
        n_rows, width = hidden.shape
        full_width = width * tp_size
        block_rows = emb_table.shape[0]
        block = block_rows // tp_size
        chunk = chunk_of(block)
        n_chunks = block // chunk
        n_dev = tp_size * vp_size

        local_idx = next_tok - lax.axis_index("vp") * block_rows
        is_owned = (local_idx >= 0) & (local_idx < block_rows)
        picked = jnp.take(emb_table, jnp.clip(local_idx, 0, block_rows - 1), axis=0).astype(jnp.float32)
        picked = jnp.where(is_owned[:, None], picked, jnp.zeros_like(picked))

        dma = pltpu.SemaphoreType.DMA
        vmem = pl.BlockSpec(memory_space=pltpu.VMEM)
        z, ls, next_in = pl.pallas_call(
            functools.partial(main_kernel, vp_size, chunk, n_chunks, full_width),
            out_shape=(
                jax.ShapeDtypeStruct((n_rows, block), jnp.float32),
                jax.ShapeDtypeStruct((n_rows, LANES // 2), jnp.float32),
                jax.ShapeDtypeStruct((n_rows, width), jnp.bfloat16),
            ),
            in_specs=[vmem, vmem, vmem, pl.BlockSpec(memory_space=pl.ANY), vmem, vmem, vmem],
            out_specs=(vmem, vmem, vmem),
            scratch_shapes=[
                pltpu.VMEM((SLOTS, 2, chunk, width), jnp.bfloat16),
                pltpu.VMEM((n_rows, width), jnp.bfloat16),
                pltpu.VMEM((2 * n_chunks, n_rows, chunk), jnp.float32),
                pltpu.VMEM((2 * n_chunks, n_rows, chunk), jnp.float32),
                pltpu.VMEM((2 * n_chunks, n_rows, chunk), jnp.float32),
                pltpu.VMEM((n_chunks, n_rows, chunk), jnp.float32),
                pltpu.VMEM((tp_size, n_rows, LANES), jnp.float32),
                pltpu.VMEM((max(vp_size - 1, 1), n_rows, width), jnp.float32),
                pltpu.VMEM((tp_size, n_rows, LANES), jnp.float32),
                pltpu.VMEM((n_dev, n_rows, LANES), jnp.float32),
                dma((SLOTS, 2)),
                dma((2 * n_chunks,)),
                dma((2 * n_chunks,)),
                dma((n_chunks,)),
                dma((n_chunks,)),
                dma((tp_size - 1,)),
                dma((tp_size - 1,)),
                dma((max(vp_size - 1, 1),)),
                dma((max(vp_size - 1, 1),)),
                dma((tp_size - 1,)),
                dma((tp_size - 1,)),
                dma((n_dev - 1,)),
                dma((n_dev - 1,)),
            ],
            compiler_params=pltpu.CompilerParams(collective_id=0, has_side_effects=True),
        )(
            hidden, lnf_gain.reshape(1, width), lnf_bias.reshape(1, width), emb_table, picked,
            eln_gain.reshape(1, width), eln_bias.reshape(1, width),
        )
        log_sum = ls[:, 0]
        logprobs = z - log_sum[:, None]
        return logprobs, log_sum, next_in

    return jax.shard_map(
        per_device,
        mesh=mesh,
        in_specs=(P("dp", "tp"), P("tp"), P("tp"), P("vp", "tp"), P("dp"), P("tp"), P("tp")),
        out_specs=(P("dp", ("vp", "tp")), P("dp"), P("dp", "tp")),
        check_vma=False,
    )
```

```python
import functools

import jax
import jax.numpy as jnp
from jax import lax
from jax.experimental import pallas as pl
from jax.experimental.pallas import tpu as pltpu
from jax.sharding import PartitionSpec as P

NORM_EPS = 1e-5
MESH = pl.DeviceIdType.MESH
LANES = 128
CHUNK = 1792
SLOTS = 4
OUT_PARTS = 7


def row_sums(rows_f32):
    return jnp.sum(rows_f32, axis=1, keepdims=True), jnp.sum(rows_f32 * rows_f32, axis=1, keepdims=True)


def pack_lanes(columns):
    shape = (columns[0].shape[0], LANES)
    lane = lax.broadcasted_iota(jnp.int32, shape, 1)
    span = LANES // len(columns)
    packed = jnp.broadcast_to(columns[0], shape)
    for i, column in enumerate(columns[1:], 1):
        packed = jnp.where(lane >= i * span, jnp.broadcast_to(column, shape), packed)
    return packed


def apply_norm(rows_f32, sums, squares, gain, bias, full_width):
    mean = sums / full_width
    var = squares / full_width - mean * mean
    scaled = (rows_f32 - mean) * lax.rsqrt(var + NORM_EPS)
    return (scaled * gain + bias).astype(jnp.bfloat16)


def main_kernel(
    vp_size, first, n_chunks, full_width,
    hid_hbm, g1_hbm, b1_hbm, table_ref, tok_hbm, g2_hbm, b2_hbm,
    z_ref, sums_ref, rows_ref, affine_ref,
    hid_ref, g1_ref, b1_ref, tok_ref, tab, xn, mine, give, take, land, mine0, give0, take0, land0,
    st, row_own, row_in, fs,
    in_sem, tab_sem, give_sem, take_sem, push_sem, land_sem, st_ssem, st_rsem, row_ssem, row_rsem, fs_ssem, fs_rsem,
):
    v = lax.axis_index("vp")
    t = lax.axis_index("tp")
    n_dev = vp_size * 4
    me = v * 4 + t
    core = t % 2
    chip = t // 2
    sib = chip * 2 + 1 - core
    across = (1 - chip) * 2 + core
    diag = (1 - chip) * 2 + 1 - core
    block = first + CHUNK * n_chunks

    barrier = pltpu.get_barrier_semaphore()
    for d in range(1, n_dev):
        other = (me + d) % n_dev
        pl.semaphore_signal(barrier, inc=1, device_id={"vp": other // 4, "tp": other % 4}, device_id_type=MESH)

    small = [
        pltpu.make_async_copy(src, dst, in_sem.at[i])
        for i, (src, dst) in enumerate((
            (hid_hbm, hid_ref), (g1_hbm, g1_ref), (b1_hbm, b1_ref), (tok_hbm, tok_ref),
            (g2_hbm, affine_ref.at[pl.ds(0, 1)]), (b2_hbm, affine_ref.at[pl.ds(1, 1)]),
        ))
    ]
    for copy in small:
        copy.start()

    def table_start(phase, step, part):
        owner_chip = (1 - chip) if phase == 0 else chip
        owner_core = (1 - core) if part == 0 else core
        base = (owner_chip * 2 + owner_core) * block
        return base if isinstance(step, int) and step == 0 else base + first + (step - 1) * CHUNK

    def table_copy(phase, step, slot, part):
        size = first if isinstance(step, int) and step == 0 else CHUNK
        start = pl.multiple_of(table_start(phase, step, part), LANES)
        return pltpu.make_async_copy(
            table_ref.at[pl.ds(start, size), :], tab.at[slot, part, pl.ds(0, size)], tab_sem.at[slot, part]
        )

    per_phase = n_chunks + 1

    def prefetch(phase, step):
        slot = (phase * per_phase + step) % SLOTS
        for part in range(2):
            table_copy(phase, step, slot, part).start()

    for s in range(SLOTS):
        prefetch(0, s)

    small[0].wait()
    hid = hid_ref[...].astype(jnp.float32)
    st[t] = pack_lanes(row_sums(hid))
    pl.semaphore_wait(barrier, n_dev - 1)

    stat_copies = []
    for i, target in enumerate((across, diag, sib)):
        copy = pltpu.make_async_remote_copy(
            st.at[t], st.at[t], st_ssem.at[i], st_rsem.at[i], device_id={"tp": target}, device_id_type=MESH
        )
        copy.start()
        stat_copies.append(copy)

    for copy in small[1:]:
        copy.wait()
    n_rows = hid.shape[0]
    on_diag = lax.broadcasted_iota(jnp.int32, (n_rows, n_rows), 0) == lax.broadcasted_iota(jnp.int32, (n_rows, n_rows), 1)
    tok_f32 = jnp.broadcast_to(tok_ref[...].astype(jnp.float32), (n_rows, n_rows))
    tok_col = jnp.sum(jnp.where(on_diag, tok_f32, 0.0), axis=1, keepdims=True).astype(jnp.int32)
    tok_col = tok_col - v * (4 * block)
    row_own[...] = jnp.zeros_like(row_own)

    for copy in stat_copies:
        copy.wait_recv()
    total = st[0] + st[1] + st[2] + st[3]
    half = LANES // 2
    xn[...] = apply_norm(hid, total[:, 0:1], total[:, half : half + 1], g1_ref[...], b1_ref[...], full_width)

    def bufs(phase, step):
        if isinstance(step, int) and step == 0:
            return mine0.at[phase], give0.at[phase], take0.at[phase], land0, phase * per_phase
        i = phase * n_chunks + step - 1
        return mine.at[i], give.at[i], take.at[i], land.at[step - 1], phase * per_phase + step

    def give_copy(phase, step):
        _, src, dst, _, k = bufs(phase, step)
        return pltpu.make_async_remote_copy(
            src, dst, give_sem.at[k], take_sem.at[k], device_id={"tp": sib}, device_id_type=MESH
        )

    def push_copy(step):
        src, _, _, dst, k = bufs(0, step)
        return pltpu.make_async_remote_copy(
            src, dst, push_sem.at[k], land_sem.at[k], device_id={"tp": across}, device_id_type=MESH
        )

    def combine(phase, step):
        own, _, got, _, _ = bufs(phase, step)
        give_copy(phase, step).wait_recv()
        own[...] = own[...] + got[...]
        if phase == 0:
            push_copy(step).start()

    def produce(phase, step, select=True):
        size = first if isinstance(step, int) and step == 0 else CHUNK
        slot = (phase * per_phase + step) % SLOTS
        own, out, _, _, _ = bufs(phase, step)
        for part, dst in enumerate((out, own)):
            table_copy(phase, step, slot, part).wait()
            dst[...] = lax.dot_general(
                xn[...], tab[slot, part, 0:size, :], (((1,), (1,)), ((), ())), preferred_element_type=jnp.float32
            )
            if select:
                select_part(phase, step, part)
            if part == 0:
                give_copy(phase, step).start()

    def select_part(phase, step, part):
        size = first if isinstance(step, int) and step == 0 else CHUNK
        slot = (phase * per_phase + step) % SLOTS
        at = tok_col - table_start(phase, step, part)
        hit = lax.broadcasted_iota(jnp.int32, (n_rows, size), 1) == at
        ones = jnp.where(hit, 1.0, 0.0).astype(jnp.bfloat16)
        row_own[...] = row_own[...] + jnp.dot(ones, tab[slot, part, 0:size, :], preferred_element_type=jnp.float32)

    produce(0, 0, select=False)
    produce(0, 1, select=False)
    combine(0, 0)
    for step in range(2):
        for part in range(2):
            select_part(0, step, part)
        prefetch(0, SLOTS + step)

    def far_step(step, carry, next_phase=0):
        produce(0, step)
        combine(0, step - 1)
        prefetch(next_phase, step + SLOTS - next_phase * per_phase)
        return carry

    lax.fori_loop(2, per_phase - SLOTS, far_step, 0)
    produce(0, per_phase - SLOTS)
    combine(0, per_phase - SLOTS - 1)
    prefetch(1, 0)
    lax.fori_loop(per_phase - SLOTS + 1, per_phase, functools.partial(far_step, next_phase=1), 0)

    produce(1, 0)
    combine(0, n_chunks)
    prefetch(1, SLOTS)
    produce(1, 1)
    combine(1, 0)
    prefetch(1, SLOTS + 1)

    def near_step(step, carry):
        produce(1, step)
        combine(1, step - 1)

        @pl.when(step + SLOTS < per_phase)
        def _():
            prefetch(1, step + SLOTS)

        return carry

    lax.fori_loop(2, per_phase, near_step, 0)

    row_copies = []
    for d in range(1, vp_size):
        copy = pltpu.make_async_remote_copy(
            row_own, row_in.at[d - 1], row_ssem.at[d - 1], row_rsem.at[d - 1],
            device_id={"vp": (v + d) % vp_size}, device_id_type=MESH,
        )
        copy.start()
        row_copies.append(copy)
    combine(1, n_chunks)
    own_sums, own_squares = row_sums(row_own[...])

    def finish(step, carry):
        size, offset = (first, 0) if isinstance(step, int) and step == 0 else (CHUNK, first + (step - 1) * CHUNK)
        top, acc = carry
        own, _, _, _, _ = bufs(1, step)
        _, _, _, got, _ = bufs(0, step)
        push_copy(step).wait_recv()
        vals = own[...] + got[...]
        z_ref[:, pl.ds(pl.multiple_of(offset, LANES), size)] = vals
        tiles = [vals[:, i * LANES : (i + 1) * LANES] for i in range(size // LANES)]
        new_top = functools.reduce(jnp.maximum, tiles, top)
        acc = acc * jnp.exp(top - new_top)
        for tile in tiles:
            acc = acc + jnp.exp(tile - new_top)
        return new_top, acc

    state = (jnp.full((n_rows, LANES), -jnp.inf, jnp.float32), jnp.zeros((n_rows, LANES), jnp.float32))
    state = finish(0, state)
    top, acc = lax.fori_loop(1, per_phase, finish, state)
    row_top = jnp.max(top, axis=1, keepdims=True)
    row_sum = jnp.sum(acc * jnp.exp(top - row_top), axis=1, keepdims=True)
    fs[me] = pack_lanes((row_top, row_sum, own_sums, own_squares))
    last_copies = []
    for d in range(1, n_dev):
        other = (me + d) % n_dev
        copy = pltpu.make_async_remote_copy(
            fs.at[me], fs.at[me], fs_ssem.at[d - 1], fs_rsem.at[d - 1],
            device_id={"vp": other // 4, "tp": other % 4}, device_id_type=MESH,
        )
        copy.start()
        last_copies.append(copy)

    rows = row_own[...]
    for d in range(1, vp_size):
        row_copies[d - 1].wait_recv()
        rows = rows + row_in[d - 1]
    rows_ref[...] = rows
    for copy in stat_copies + row_copies:
        copy.wait_send()
    for phase in range(2):
        give_copy(phase, 0).wait_send()

        def drain(step, carry, phase=phase):
            give_copy(phase, step).wait_send()
            if phase == 0:
                push_copy(step).wait_send()
            return carry

        lax.fori_loop(1, per_phase, drain, 0)
    push_copy(0).wait_send()

    for copy in last_copies:
        copy.wait()
    sums_ref[...] = fs[...]


def tail_kernel(
    n_dev, full_width, z_ref, sums_ref, rows_ref, affine_ref, out_hbm, ls_hbm, nxt_hbm, out, ls, nxt, sem
):
    quarter = LANES // 4
    packed = [sums_ref[i] for i in range(n_dev)]
    all_top = functools.reduce(jnp.maximum, [p[:, 0:1] for p in packed])
    all_sum = functools.reduce(jnp.add, [p[:, quarter : quarter + 1] * jnp.exp(p[:, 0:1] - all_top) for p in packed])
    log_sum = all_top + jnp.log(all_sum)
    n_rows, block = out.shape
    part = block // OUT_PARTS
    copies = []
    for i in range(OUT_PARTS):
        columns = pl.ds(i * part, part)
        out[:, columns] = z_ref[:, columns] - log_sum
        copy = pltpu.make_async_copy(out.at[:, columns], out_hbm.at[:, columns], sem.at[i])
        copy.start()
        copies.append(copy)
    on_diag = lax.broadcasted_iota(jnp.int32, (n_rows, n_rows), 0) == lax.broadcasted_iota(jnp.int32, (n_rows, n_rows), 1)
    ls[...] = jnp.sum(jnp.where(on_diag, jnp.broadcast_to(log_sum, (n_rows, n_rows)), 0.0), axis=0, keepdims=True)
    copy = pltpu.make_async_copy(ls, ls_hbm, sem.at[OUT_PARTS])
    copy.start()
    copies.append(copy)
    sums = functools.reduce(jnp.add, [p[:, 2 * quarter : 2 * quarter + 1] for p in packed])
    squares = functools.reduce(jnp.add, [p[:, 3 * quarter : 3 * quarter + 1] for p in packed])
    nxt[...] = apply_norm(rows_ref[...], sums, squares, affine_ref[0:1, :], affine_ref[1:2, :], full_width)
    copy = pltpu.make_async_copy(nxt, nxt_hbm, sem.at[OUT_PARTS + 1])
    copy.start()
    copies.append(copy)
    for copy in copies:
        copy.wait()


def solution(mesh):
    tp_size = mesh.shape["tp"]
    vp_size = mesh.shape["vp"]
    n_dev = tp_size * vp_size

    def per_device(hidden, lnf_gain, lnf_bias, emb_table, next_tok, eln_gain, eln_bias):
        n_rows, width = hidden.shape
        full_width = width * tp_size
        block = emb_table.shape[0] // tp_size
        n_chunks = block // CHUNK
        first = block - n_chunks * CHUNK
        per_phase = n_chunks + 1

        dma = pltpu.SemaphoreType.DMA
        f32 = jnp.float32
        hbm = pl.BlockSpec(memory_space=pl.ANY)
        vmem = pl.BlockSpec(memory_space=pltpu.VMEM)
        row = lambda a: a.reshape(1, a.shape[0])
        z, sums, rows, affine = pl.pallas_call(
            functools.partial(main_kernel, vp_size, first, n_chunks, full_width),
            out_shape=(
                pltpu.VMEM((n_rows, block), f32),
                pltpu.VMEM((n_dev, n_rows, LANES), f32),
                pltpu.VMEM((n_rows, width), f32),
                pltpu.VMEM((2, width), f32),
            ),
            in_specs=[pl.BlockSpec(memory_space=pltpu.HBM)] * 7,
            out_specs=(vmem,) * 4,
            scratch_shapes=[
                pltpu.VMEM((n_rows, width), jnp.bfloat16),
                pltpu.VMEM((1, width), f32),
                pltpu.VMEM((1, width), f32),
                pltpu.VMEM((1, n_rows), jnp.int32),
                pltpu.VMEM((SLOTS, 2, CHUNK, width), jnp.bfloat16),
                pltpu.VMEM((n_rows, width), jnp.bfloat16),
                pltpu.VMEM((2 * n_chunks, n_rows, CHUNK), f32),
                pltpu.VMEM((2 * n_chunks, n_rows, CHUNK), f32),
                pltpu.VMEM((2 * n_chunks, n_rows, CHUNK), f32),
                pltpu.VMEM((n_chunks, n_rows, CHUNK), f32),
                pltpu.VMEM((2, n_rows, first), f32),
                pltpu.VMEM((2, n_rows, first), f32),
                pltpu.VMEM((2, n_rows, first), f32),
                pltpu.VMEM((n_rows, first), f32),
                pltpu.VMEM((tp_size, n_rows, LANES), f32),
                pltpu.VMEM((n_rows, width), f32),
                pltpu.VMEM((vp_size - 1, n_rows, width), f32),
                pltpu.VMEM((n_dev, n_rows, LANES), f32),
                dma((6,)),
                dma((SLOTS, 2)),
                dma((2 * per_phase,)),
                dma((2 * per_phase,)),
                dma((per_phase,)),
                dma((per_phase,)),
                dma((tp_size - 1,)),
                dma((tp_size - 1,)),
                dma((vp_size - 1,)),
                dma((vp_size - 1,)),
                dma((n_dev - 1,)),
                dma((n_dev - 1,)),
            ],
            compiler_params=pltpu.CompilerParams(
                collective_id=0, has_side_effects=True, vmem_limit_bytes=40 * 2**20
            ),
        )(*(
            pltpu.with_memory_space_constraint(a, pltpu.HBM)
            for a in (hidden, row(lnf_gain), row(lnf_bias), emb_table, row(next_tok), row(eln_gain), row(eln_bias))
        ))
        logprobs, log_sum, next_in = pl.pallas_call(
            functools.partial(tail_kernel, n_dev, full_width),
            out_shape=(
                jax.ShapeDtypeStruct((n_rows, block), f32),
                jax.ShapeDtypeStruct((1, n_rows), f32),
                jax.ShapeDtypeStruct((n_rows, width), jnp.bfloat16),
            ),
            in_specs=[vmem] * 4,
            out_specs=(hbm,) * 3,
            scratch_shapes=[
                pltpu.VMEM((n_rows, block), f32),
                pltpu.VMEM((1, n_rows), f32),
                pltpu.VMEM((n_rows, width), jnp.bfloat16),
                dma((OUT_PARTS + 2,)),
            ],
            compiler_params=pltpu.CompilerParams(vmem_limit_bytes=12 * 2**20),
        )(*(pltpu.with_memory_space_constraint(a, pltpu.VMEM) for a in (z, sums, rows, affine)))
        return logprobs, log_sum.reshape(n_rows), next_in

    return jax.shard_map(
        per_device,
        mesh=mesh,
        in_specs=(P("dp", "tp"), P("tp"), P("tp"), P("vp", "tp"), P("dp"), P("tp"), P("tp")),
        out_specs=(P("dp", ("vp", "tp")), P("dp"), P("dp", "tp")),
        check_vma=False,
    )
```

```python
import functools

import jax
import jax.numpy as jnp
from jax import lax
from jax.experimental import pallas as pl
from jax.experimental.pallas import tpu as pltpu
from jax.sharding import PartitionSpec as P

NORM_EPS = 1e-5
MESH = pl.DeviceIdType.MESH
LANES = 128
SUBLANES = 8
CHUNK = 1792
SMALL = (640, 1024, 1024)
SLOTS = 4
TAKES = 4
OUT_PARTS = 7


def row_sums(rows_f32):
    return jnp.sum(rows_f32, axis=1, keepdims=True), jnp.sum(rows_f32 * rows_f32, axis=1, keepdims=True)


def pack_lanes(columns):
    halves = [c[i * SUBLANES : (i + 1) * SUBLANES] for c in columns for i in range(2)]
    shape = (SUBLANES, LANES)
    lane = lax.broadcasted_iota(jnp.int32, shape, 1)
    span = LANES // len(halves)
    packed = jnp.broadcast_to(halves[0], shape)
    for i, column in enumerate(halves[1:], 1):
        packed = jnp.where(lane >= i * span, jnp.broadcast_to(column, shape), packed)
    return packed


def unpack_lanes(packed, i, n_columns):
    span = LANES // (2 * n_columns)
    at = 2 * i * span
    return jnp.concatenate([packed[:, at : at + 1], packed[:, at + span : at + span + 1]], axis=0)


def apply_norm(rows_f32, sums, squares, gain, bias, full_width):
    mean = sums / full_width
    var = squares / full_width - mean * mean
    scaled = (rows_f32 - mean) * lax.rsqrt(var + NORM_EPS)
    return (scaled * gain + bias).astype(jnp.bfloat16)


def main_kernel(
    vp_size, sizes, shared, full_width,
    hid_hbm, g1_hbm, b1_hbm, table_ref, tok_hbm, g2_hbm, b2_hbm,
    z_ref, sums_ref, rows_ref, affine_ref,
    hid_ref, g1_ref, b1_ref, tok_ref, tab, xn, push, give, take, land, land_diag, st, row_own, row_in, fs,
    in_sem, tab_sem, give_sem, take_sem, push_sem, land_sem, diag_sem,
    st_ssem, st_rsem, row_ssem, row_rsem, fs_ssem, fs_rsem,
):
    v = lax.axis_index("vp")
    t = lax.axis_index("tp")
    n_dev = vp_size * 4
    me = v * 4 + t
    core = t % 2
    chip = t // 2
    sib = chip * 2 + 1 - core
    across = (1 - chip) * 2 + core
    diag = (1 - chip) * 2 + 1 - core
    n_rows, block = z_ref.shape
    n_small = len(SMALL)
    n_steps = len(sizes)

    barrier = pltpu.get_barrier_semaphore()
    for d in range(1, n_dev):
        other = (me + d) % n_dev
        pl.semaphore_signal(barrier, inc=1, device_id={"vp": other // 4, "tp": other % 4}, device_id_type=MESH)

    def wait_sends(ref, sem):
        pltpu.make_async_remote_copy(
            ref, ref, sem, st_rsem.at[0], device_id={"tp": sib}, device_id_type=MESH
        ).wait_send()

    def wait_arrivals(ref, sem):
        pltpu.make_async_remote_copy(
            ref, ref, st_ssem.at[0], sem, device_id={"tp": sib}, device_id_type=MESH
        ).wait_recv()

    small = [
        pltpu.make_async_copy(src, dst, in_sem.at[i])
        for i, (src, dst) in enumerate((
            (hid_hbm, hid_ref), (g1_hbm, g1_ref), (b1_hbm, b1_ref), (tok_hbm, tok_ref),
            (g2_hbm, affine_ref.at[pl.ds(0, 1)]), (b2_hbm, affine_ref.at[pl.ds(1, 1)]),
        ))
    ]
    for copy in small:
        copy.start()

    def columns(step):
        if isinstance(step, int):
            return pl.ds(sum(sizes[:step]), sizes[step])
        return pl.ds(pl.multiple_of(sum(sizes[:n_small]) + (step - n_small) * CHUNK, LANES), CHUNK)

    def table_rows(phase, step, part):
        owner_chip = (1 - chip) if phase == 0 else chip
        owner_core = (1 - core) if part == 0 else core
        where = columns(step)
        return pl.ds(pl.multiple_of((owner_chip * 2 + owner_core) * block + where.start, LANES), where.size)

    def table_copy(phase, step, part):
        slot = (phase * n_steps + step) % SLOTS
        where = table_rows(phase, step, part)
        return pltpu.make_async_copy(
            table_ref.at[where, :], tab.at[slot, part, pl.ds(0, where.size)], tab_sem.at[slot, part]
        )

    def prefetch(phase, step):
        for part in range(2):
            table_copy(phase, step, part).start()

    for s in range(SLOTS):
        prefetch(0, s)

    small[0].wait()
    hid = hid_ref[...].astype(jnp.float32)
    st[t] = pack_lanes(row_sums(hid))
    pl.semaphore_wait(barrier, n_dev - 1)

    for target in (across, diag, sib):
        copy = pltpu.make_async_remote_copy(
            st.at[t], st.at[t], st_ssem.at[0], st_rsem.at[0], device_id={"tp": target}, device_id_type=MESH
        )
        copy.start()

    for copy in small[1:]:
        copy.wait()
    square = (n_rows, n_rows)
    on_diag = lax.broadcasted_iota(jnp.int32, square, 0) == lax.broadcasted_iota(jnp.int32, square, 1)
    tok_f32 = jnp.broadcast_to(tok_ref[...].astype(jnp.float32), square)
    tok_col = jnp.sum(jnp.where(on_diag, tok_f32, 0.0), axis=1, keepdims=True).astype(jnp.int32)
    tok_col = tok_col - v * (4 * block)
    row_own[...] = jnp.zeros_like(row_own)

    wait_arrivals(st.at[pl.ds(0, 3)], st_rsem.at[0])
    total = st[0] + st[1] + st[2] + st[3]
    xn[...] = apply_norm(
        hid, unpack_lanes(total, 0, 2), unpack_lanes(total, 1, 2), g1_ref[...], b1_ref[...], full_width
    )

    def give_copy(phase, step):
        where = columns(step)
        return pltpu.make_async_remote_copy(
            give.at[phase, :, where], take.at[phase, :, where], give_sem.at[0],
            take_sem.at[(phase * n_steps + step) % TAKES], device_id={"tp": sib}, device_id_type=MESH,
        )

    def push_copy(step, sem):
        where = columns(step)
        return pltpu.make_async_remote_copy(
            push.at[:, where], land.at[:, where], push_sem.at[0], land_sem.at[sem],
            device_id={"tp": across}, device_id_type=MESH,
        )

    def diag_copy():
        return pltpu.make_async_remote_copy(
            give.at[0, :, columns(0)], land_diag, give_sem.at[0], diag_sem.at[0],
            device_id={"tp": diag}, device_id_type=MESH,
        )

    def combine(phase, step, sem=None):
        where = columns(step)
        give_copy(phase, step).wait_recv()
        own = push if phase == 0 else z_ref
        own[:, where] = own[:, where] + take[phase, :, where]
        if phase == 0:
            push_copy(step, sem).start()

    def produce(phase, step, select=True):
        where = columns(step)
        slot = (phase * n_steps + step) % SLOTS
        for part in range(2):
            table_copy(phase, step, part).wait()
            vals = lax.dot_general(
                xn[...], tab[slot, part, 0 : where.size, :], (((1,), (1,)), ((), ())), preferred_element_type=jnp.float32
            )
            if part == 0:
                give[phase, :, where] = vals
            elif phase == 0:
                push[:, where] = vals
            else:
                z_ref[:, where] = vals
            if select:
                select_part(phase, step, part)
            if part == 0 and phase == 0 and isinstance(step, int) and step == 0:
                diag_copy().start()
            elif part == 0:
                give_copy(phase, step).start()

    def select_part(phase, step, part):
        where = table_rows(phase, step, part)
        slot = (phase * n_steps + step) % SLOTS
        hit = lax.broadcasted_iota(jnp.int32, (n_rows, where.size), 1) == tok_col - where.start
        ones = jnp.where(hit, 1.0, 0.0).astype(jnp.bfloat16)
        row_own[...] = row_own[...] + jnp.dot(
            ones, tab[slot, part, 0 : where.size, :], preferred_element_type=jnp.float32
        )

    produce(0, 0, select=False)
    push_copy(0, 0).start()
    produce(0, 1, select=False)
    produce(0, 2, select=False)

    def early_rows():
        for step in range(3):
            for part in range(2):
                select_part(0, step, part)

    pl.when(core == 1)(early_rows)
    combine(0, 1, 1)
    pl.when(core == 0)(early_rows)
    for step in range(3):
        prefetch(0, SLOTS + step)

    def far_step(step, carry):
        produce(0, step)
        combine(0, step - 1, 1)
        prefetch(0, step + SLOTS)
        return carry

    far_step(n_small, 0)
    lax.fori_loop(n_small + 1, n_steps - SLOTS, far_step, 0)
    for step in range(n_steps - SLOTS, n_steps):
        produce(0, step)
        combine(0, step - 1, max(step - 1 - shared, 0) + 1)
        prefetch(1, step + SLOTS - n_steps)

    for step in range(n_small + 1):
        produce(1, step)
        combine(0, n_steps - 1, n_steps - shared) if step == 0 else combine(1, step - 1)
        prefetch(1, SLOTS + step)

    def near_step(step, carry):
        produce(1, step)
        combine(1, step - 1)

        @pl.when(step + SLOTS < n_steps)
        def _():
            prefetch(1, step + SLOTS)

        return carry

    lax.fori_loop(n_small + 1, n_steps, near_step, 0)

    row_copies = []
    for d in range(1, vp_size):
        copy = pltpu.make_async_remote_copy(
            row_own, row_in.at[d - 1], row_ssem.at[d - 1], row_rsem.at[d - 1],
            device_id={"vp": (v + d) % vp_size}, device_id_type=MESH,
        )
        copy.start()
        row_copies.append(copy)
    combine(1, n_steps - 1)
    own_sums, own_squares = row_sums(row_own[...])

    def finish(step, carry, own_sem=False):
        where = columns(step)
        top, acc = carry
        if own_sem:
            push_copy(step, step - shared + 1).wait_recv()
        vals = z_ref[:, where] + land[:, where]
        if isinstance(step, int) and step == 0:
            vals = vals + land_diag[...]
        z_ref[:, where] = vals
        tiles = [vals[:, i * LANES : (i + 1) * LANES] for i in range(where.size // LANES)]
        new_top = functools.reduce(jnp.maximum, tiles, top)
        acc = acc * jnp.exp(top - new_top)
        for tile in tiles:
            acc = acc + jnp.exp(tile - new_top)
        return new_top, acc

    state = (jnp.full((n_rows, LANES), -jnp.inf, jnp.float32), jnp.zeros((n_rows, LANES), jnp.float32))
    push_copy(0, 0).wait_recv()
    diag_copy().wait_recv()
    together = land.at[:, pl.ds(sizes[0], sum(sizes[1 : shared + 1]))]
    wait_arrivals(together, land_sem.at[1])
    for step in range(n_small):
        state = finish(step, state)
    state = lax.fori_loop(n_small, shared + 1, finish, state)
    top, acc = lax.fori_loop(shared + 1, n_steps, functools.partial(finish, own_sem=True), state)
    row_top = jnp.max(top, axis=1, keepdims=True)
    row_sum = jnp.sum(acc * jnp.exp(top - row_top), axis=1, keepdims=True)
    fs[me] = pack_lanes((row_top, row_sum, own_sums, own_squares))
    for d in range(1, n_dev):
        other = (me + d) % n_dev
        copy = pltpu.make_async_remote_copy(
            fs.at[me], fs.at[me], fs_ssem.at[0], fs_rsem.at[0],
            device_id={"vp": other // 4, "tp": other % 4}, device_id_type=MESH,
        )
        copy.start()

    rows = row_own[...]
    for d in range(1, vp_size):
        row_copies[d - 1].wait_recv()
        rows = rows + row_in[d - 1]
    rows_ref[...] = rows
    for copy in row_copies:
        copy.wait_send()
    wait_sends(st.at[pl.ds(0, 3)], st_ssem.at[0])
    wait_sends(give, give_sem.at[0])
    wait_sends(push, push_sem.at[0])
    wait_arrivals(fs.at[pl.ds(0, n_dev - 1)], fs_rsem.at[0])
    wait_sends(fs.at[pl.ds(0, n_dev - 1)], fs_ssem.at[0])
    sums_ref[...] = fs[...]


def tail_kernel(
    n_dev, full_width, z_ref, sums_ref, rows_ref, affine_ref, out_hbm, ls_hbm, nxt_hbm, out, ls, nxt, sem
):
    packed = [sums_ref[i] for i in range(n_dev)]
    tops = [unpack_lanes(p, 0, 4) for p in packed]
    all_top = functools.reduce(jnp.maximum, tops)
    all_sum = functools.reduce(jnp.add, [unpack_lanes(p, 1, 4) * jnp.exp(m - all_top) for p, m in zip(packed, tops)])
    log_sum = all_top + jnp.log(all_sum)
    n_rows, block = out.shape
    part = block // OUT_PARTS
    for i in range(OUT_PARTS):
        columns = pl.ds(i * part, part)
        out[:, columns] = z_ref[:, columns] - log_sum
        pltpu.make_async_copy(out.at[:, columns], out_hbm.at[:, columns], sem.at[0]).start()
    square = (n_rows, n_rows)
    on_diag = lax.broadcasted_iota(jnp.int32, square, 0) == lax.broadcasted_iota(jnp.int32, square, 1)
    ls[...] = jnp.sum(jnp.where(on_diag, jnp.broadcast_to(log_sum, square), 0.0), axis=0, keepdims=True)
    ls_copy = pltpu.make_async_copy(ls, ls_hbm, sem.at[1])
    ls_copy.start()
    sums = functools.reduce(jnp.add, [unpack_lanes(p, 2, 4) for p in packed])
    squares = functools.reduce(jnp.add, [unpack_lanes(p, 3, 4) for p in packed])
    nxt[...] = apply_norm(rows_ref[...], sums, squares, affine_ref[0:1, :], affine_ref[1:2, :], full_width)
    nxt_copy = pltpu.make_async_copy(nxt, nxt_hbm, sem.at[2])
    nxt_copy.start()
    pltpu.make_async_copy(out, out_hbm, sem.at[0]).wait()
    ls_copy.wait()
    nxt_copy.wait()


def solution(mesh):
    tp_size = mesh.shape["tp"]
    vp_size = mesh.shape["vp"]
    n_dev = tp_size * vp_size

    def per_device(hidden, lnf_gain, lnf_bias, emb_table, next_tok, eln_gain, eln_bias):
        n_rows, width = hidden.shape
        full_width = width * tp_size
        block = emb_table.shape[0] // tp_size
        sizes = SMALL + (CHUNK,) * ((block - sum(SMALL)) // CHUNK)
        assert sum(sizes) == block
        shared = len(sizes) - SLOTS - 1

        dma = pltpu.SemaphoreType.DMA
        f32 = jnp.float32
        hbm = pl.BlockSpec(memory_space=pltpu.HBM)
        vmem = pl.BlockSpec(memory_space=pltpu.VMEM)
        row = lambda a: a.reshape(1, a.shape[0])
        z, sums, rows, affine = pl.pallas_call(
            functools.partial(main_kernel, vp_size, sizes, shared, full_width),
            out_shape=(
                pltpu.VMEM((n_rows, block), f32),
                pltpu.VMEM((n_dev, SUBLANES, LANES), f32),
                pltpu.VMEM((n_rows, width), f32),
                pltpu.VMEM((2, width), f32),
            ),
            in_specs=[hbm] * 7,
            out_specs=(vmem,) * 4,
            scratch_shapes=[
                pltpu.VMEM((n_rows, width), jnp.bfloat16),
                pltpu.VMEM((1, width), f32),
                pltpu.VMEM((1, width), f32),
                pltpu.VMEM((1, n_rows), jnp.int32),
                pltpu.VMEM((SLOTS, 2, CHUNK, width), jnp.bfloat16),
                pltpu.VMEM((n_rows, width), jnp.bfloat16),
                pltpu.VMEM((n_rows, block), f32),
                pltpu.VMEM((2, n_rows, block), f32),
                pltpu.VMEM((2, n_rows, block), f32),
                pltpu.VMEM((n_rows, block), f32),
                pltpu.VMEM((n_rows, SMALL[0]), f32),
                pltpu.VMEM((tp_size, SUBLANES, LANES), f32),
                pltpu.VMEM((n_rows, width), f32),
                pltpu.VMEM((vp_size - 1, n_rows, width), f32),
                pltpu.VMEM((n_dev, SUBLANES, LANES), f32),
                dma((6,)),
                dma((SLOTS, 2)),
                dma((1,)),
                dma((TAKES,)),
                dma((1,)),
                dma((len(sizes) - shared + 1,)),
                dma((1,)),
                dma((1,)),
                dma((1,)),
                dma((vp_size - 1,)),
                dma((vp_size - 1,)),
                dma((1,)),
                dma((1,)),
            ],
            compiler_params=pltpu.CompilerParams(
                collective_id=0, has_side_effects=True, vmem_limit_bytes=40 * 2**20
            ),
        )(*(
            pltpu.with_memory_space_constraint(a, pltpu.HBM)
            for a in (hidden, row(lnf_gain), row(lnf_bias), emb_table, row(next_tok), row(eln_gain), row(eln_bias))
        ))
        logprobs, log_sum, next_in = pl.pallas_call(
            functools.partial(tail_kernel, n_dev, full_width),
            out_shape=(
                jax.ShapeDtypeStruct((n_rows, block), f32),
                jax.ShapeDtypeStruct((1, n_rows), f32),
                jax.ShapeDtypeStruct((n_rows, width), jnp.bfloat16),
            ),
            in_specs=[vmem] * 4,
            out_specs=(pl.BlockSpec(memory_space=pl.ANY),) * 3,
            scratch_shapes=[
                pltpu.VMEM((n_rows, block), f32),
                pltpu.VMEM((1, n_rows), f32),
                pltpu.VMEM((n_rows, width), jnp.bfloat16),
                dma((3,)),
            ],
            compiler_params=pltpu.CompilerParams(vmem_limit_bytes=12 * 2**20),
        )(*(pltpu.with_memory_space_constraint(a, pltpu.VMEM) for a in (z, sums, rows, affine)))
        return logprobs, log_sum.reshape(n_rows), next_in

    return jax.shard_map(
        per_device,
        mesh=mesh,
        in_specs=(P("dp", "tp"), P("tp"), P("tp"), P("vp", "tp"), P("dp"), P("tp"), P("tp")),
        out_specs=(P("dp", ("vp", "tp")), P("dp"), P("dp", "tp")),
        check_vma=False,
    )
```

```python
import functools

import jax
import jax.numpy as jnp
from jax import lax
from jax.experimental import pallas as pl
from jax.experimental.pallas import tpu as pltpu
from jax.sharding import PartitionSpec as P

NORM_EPS = 1e-5
MESH = pl.DeviceIdType.MESH
LANES = 128
SUBLANES = 8
CHUNK = 1792
SMALL = (640, 1024, 1024)
SLOTS = 4
TAKES = 4
OUT_PARTS = 7


def row_sums(rows_f32):
    return jnp.sum(rows_f32, axis=1, keepdims=True), jnp.sum(rows_f32 * rows_f32, axis=1, keepdims=True)


def pack_lanes(columns):
    halves = [c[i * SUBLANES : (i + 1) * SUBLANES] for c in columns for i in range(2)]
    shape = (SUBLANES, LANES)
    lane = lax.broadcasted_iota(jnp.int32, shape, 1)
    span = LANES // len(halves)
    packed = jnp.broadcast_to(halves[0], shape)
    for i, column in enumerate(halves[1:], 1):
        packed = jnp.where(lane >= i * span, jnp.broadcast_to(column, shape), packed)
    return packed


def unpack_lanes(packed, i, n_columns):
    span = LANES // (2 * n_columns)
    at = 2 * i * span
    return jnp.concatenate([packed[:, at : at + 1], packed[:, at + span : at + span + 1]], axis=0)


def apply_norm(rows_f32, sums, squares, gain, bias, full_width):
    mean = sums / full_width
    var = squares / full_width - mean * mean
    scaled = (rows_f32 - mean) * lax.rsqrt(var + NORM_EPS)
    return (scaled * gain + bias).astype(jnp.bfloat16)


def main_kernel(
    vp_size, sizes, shared, full_width,
    hid_hbm, g1_hbm, b1_hbm, table_ref, tok_hbm, g2_hbm, b2_hbm,
    z_ref, sums_ref, rows_ref, affine_ref,
    hid_ref, g1_ref, b1_ref, tok_ref, tab, xn, push, give, take, land, land_diag, st, row_own, row_in, fs,
    in_sem, tab_sem, give_sem, take_sem, push_sem, land_sem, diag_sem,
    st_ssem, st_rsem, row_ssem, row_rsem, fs_ssem, fs_rsem,
):
    v = lax.axis_index("vp")
    t = lax.axis_index("tp")
    n_dev = vp_size * 4
    me = v * 4 + t
    core = t % 2
    chip = t // 2
    sib = chip * 2 + 1 - core
    across = (1 - chip) * 2 + core
    diag = (1 - chip) * 2 + 1 - core
    n_rows, block = z_ref.shape
    n_small = len(SMALL)
    n_steps = len(sizes)

    barrier = pltpu.get_barrier_semaphore()
    for d in range(1, n_dev):
        other = (me + d) % n_dev
        pl.semaphore_signal(barrier, inc=1, device_id={"vp": other // 4, "tp": other % 4}, device_id_type=MESH)

    def wait_sends(ref, sem):
        pltpu.make_async_remote_copy(
            ref, ref, sem, st_rsem.at[0], device_id={"tp": sib}, device_id_type=MESH
        ).wait_send()

    def wait_arrivals(ref, sem):
        pltpu.make_async_remote_copy(
            ref, ref, st_ssem.at[0], sem, device_id={"tp": sib}, device_id_type=MESH
        ).wait_recv()

    small = [
        pltpu.make_async_copy(src, dst, in_sem.at[i])
        for i, (src, dst) in enumerate((
            (hid_hbm, hid_ref), (g1_hbm, g1_ref), (b1_hbm, b1_ref), (tok_hbm, tok_ref),
            (g2_hbm, affine_ref.at[pl.ds(0, 1)]), (b2_hbm, affine_ref.at[pl.ds(1, 1)]),
        ))
    ]
    for copy in small:
        copy.start()

    def columns(step):
        if isinstance(step, int):
            return pl.ds(sum(sizes[:step]), sizes[step])
        return pl.ds(pl.multiple_of(sum(sizes[:n_small]) + (step - n_small) * CHUNK, LANES), CHUNK)

    def table_rows(phase, step, part):
        owner_chip = (1 - chip) if phase == 0 else chip
        owner_core = (1 - core) if part == 0 else core
        where = columns(step)
        return pl.ds(pl.multiple_of((owner_chip * 2 + owner_core) * block + where.start, LANES), where.size)

    def table_copy(phase, step, part):
        slot = (phase * n_steps + step) % SLOTS
        where = table_rows(phase, step, part)
        return pltpu.make_async_copy(
            table_ref.at[where, :], tab.at[slot, part, pl.ds(0, where.size)], tab_sem.at[slot, part]
        )

    def prefetch(phase, step):
        for part in range(2):
            table_copy(phase, step, part).start()

    small[0].wait()
    for s in range(SLOTS):
        prefetch(0, s)
    hid = hid_ref[...].astype(jnp.float32)
    st[t] = pack_lanes(row_sums(hid))
    pl.semaphore_wait(barrier, n_dev - 1)

    for target in (across, diag, sib):
        copy = pltpu.make_async_remote_copy(
            st.at[t], st.at[t], st_ssem.at[0], st_rsem.at[0], device_id={"tp": target}, device_id_type=MESH
        )
        copy.start()

    for copy in small[1:]:
        copy.wait()
    square = (n_rows, n_rows)
    on_diag = lax.broadcasted_iota(jnp.int32, square, 0) == lax.broadcasted_iota(jnp.int32, square, 1)
    tok_f32 = jnp.broadcast_to(tok_ref[...].astype(jnp.float32), square)
    tok_col = jnp.sum(jnp.where(on_diag, tok_f32, 0.0), axis=1, keepdims=True).astype(jnp.int32)
    tok_col = tok_col - v * (4 * block)
    row_own[...] = jnp.zeros_like(row_own)

    wait_arrivals(st.at[pl.ds(0, 3)], st_rsem.at[0])
    total = st[0] + st[1] + st[2] + st[3]
    xn[...] = apply_norm(
        hid, unpack_lanes(total, 0, 2), unpack_lanes(total, 1, 2), g1_ref[...], b1_ref[...], full_width
    )

    def give_copy(phase, step):
        where = columns(step)
        return pltpu.make_async_remote_copy(
            give.at[phase, :, where], take.at[phase, :, where], give_sem.at[0],
            take_sem.at[(phase * n_steps + step) % TAKES], device_id={"tp": sib}, device_id_type=MESH,
        )

    def push_copy(step, sem):
        where = columns(step)
        return pltpu.make_async_remote_copy(
            push.at[:, where], land.at[:, where], push_sem.at[0], land_sem.at[sem],
            device_id={"tp": across}, device_id_type=MESH,
        )

    def diag_copy():
        return pltpu.make_async_remote_copy(
            give.at[0, :, columns(0)], land_diag, give_sem.at[0], diag_sem.at[0],
            device_id={"tp": diag}, device_id_type=MESH,
        )

    def combine(phase, step, sem=None, send=True):
        where = columns(step)
        give_copy(phase, step).wait_recv()
        own = push if phase == 0 else z_ref
        own[:, where] = own[:, where] + take[phase, :, where]
        if phase == 0 and send:
            push_copy(step, sem).start()

    def produce(phase, step, select=True):
        where = columns(step)
        slot = (phase * n_steps + step) % SLOTS
        for part in range(2):
            table_copy(phase, step, part).wait()
            vals = lax.dot_general(
                xn[...], tab[slot, part, 0 : where.size, :], (((1,), (1,)), ((), ())), preferred_element_type=jnp.float32
            )
            if part == 0:
                give[phase, :, where] = vals
            elif phase == 0:
                push[:, where] = vals
            else:
                z_ref[:, where] = vals
            if select:
                select_part(phase, step, part)
            if part == 0 and phase == 0 and isinstance(step, int) and step == 0:
                diag_copy().start()
            elif part == 0:
                give_copy(phase, step).start()

    def select_part(phase, step, part):
        where = table_rows(phase, step, part)
        slot = (phase * n_steps + step) % SLOTS
        hit = lax.broadcasted_iota(jnp.int32, (n_rows, where.size), 1) == tok_col - where.start
        ones = jnp.where(hit, 1.0, 0.0).astype(jnp.bfloat16)
        row_own[...] = row_own[...] + jnp.dot(
            ones, tab[slot, part, 0 : where.size, :], preferred_element_type=jnp.float32
        )

    produce(0, 0, select=False)
    push_copy(0, 0).start()
    produce(0, 1, select=False)
    produce(0, 2, select=False)

    def early_rows():
        for step in range(3):
            for part in range(2):
                select_part(0, step, part)

    pl.when(core == 1)(early_rows)
    combine(0, 1, 1)
    pl.when(core == 0)(early_rows)
    for step in range(3):
        prefetch(0, SLOTS + step)

    def far_step(step, carry):
        produce(0, step)
        combine(0, step - 1, 1, send=False)
        hold = (core == 1) & (step >= 4) & (step < 6)

        @pl.when(jnp.logical_not(hold))
        def _():
            push_copy(step - 1, 1).start()

        @pl.when((core == 1) & (step == 6))
        def _():
            push_copy(step - 3, 1).start()
            push_copy(step - 2, 1).start()
        prefetch(0, step + SLOTS)
        return carry

    far_step(n_small, 0)
    lax.fori_loop(n_small + 1, n_steps - SLOTS, far_step, 0)
    for step in range(n_steps - SLOTS, n_steps):
        produce(0, step)
        combine(0, step - 1, max(step - 1 - shared, 0) + 1)
        prefetch(1, step + SLOTS - n_steps)

    for step in range(n_small + 1):
        produce(1, step)
        combine(0, n_steps - 1, n_steps - shared) if step == 0 else combine(1, step - 1)
        prefetch(1, SLOTS + step)

    def near_step(step, carry):
        produce(1, step)
        combine(1, step - 1)

        @pl.when(step + SLOTS < n_steps)
        def _():
            prefetch(1, step + SLOTS)

        return carry

    lax.fori_loop(n_small + 1, n_steps, near_step, 0)

    row_copies = []
    for d in range(1, vp_size):
        copy = pltpu.make_async_remote_copy(
            row_own, row_in.at[d - 1], row_ssem.at[d - 1], row_rsem.at[d - 1],
            device_id={"vp": (v + d) % vp_size}, device_id_type=MESH,
        )
        copy.start()
        row_copies.append(copy)
    combine(1, n_steps - 1)
    own_sums, own_squares = row_sums(row_own[...])

    def finish(step, carry, own_sem=False):
        where = columns(step)
        top, acc = carry
        if own_sem:
            push_copy(step, step - shared + 1).wait_recv()
        vals = z_ref[:, where] + land[:, where]
        if isinstance(step, int) and step == 0:
            vals = vals + land_diag[...]
        z_ref[:, where] = vals
        tiles = [vals[:, i * LANES : (i + 1) * LANES] for i in range(where.size // LANES)]
        new_top = functools.reduce(jnp.maximum, tiles, top)
        acc = acc * jnp.exp(top - new_top)
        for tile in tiles:
            acc = acc + jnp.exp(tile - new_top)
        return new_top, acc

    state = (jnp.full((n_rows, LANES), -jnp.inf, jnp.float32), jnp.zeros((n_rows, LANES), jnp.float32))
    push_copy(0, 0).wait_recv()
    diag_copy().wait_recv()
    together = land.at[:, pl.ds(sizes[0], sum(sizes[1 : shared + 1]))]
    wait_arrivals(together, land_sem.at[1])
    for step in range(n_small):
        state = finish(step, state)
    state = lax.fori_loop(n_small, shared + 1, finish, state)
    top, acc = lax.fori_loop(shared + 1, n_steps, functools.partial(finish, own_sem=True), state)
    row_top = jnp.max(top, axis=1, keepdims=True)
    row_sum = jnp.sum(acc * jnp.exp(top - row_top), axis=1, keepdims=True)
    fs[me] = pack_lanes((row_top, row_sum, own_sums, own_squares))
    for d in range(1, n_dev):
        other = (me + d) % n_dev
        copy = pltpu.make_async_remote_copy(
            fs.at[me], fs.at[me], fs_ssem.at[0], fs_rsem.at[0],
            device_id={"vp": other // 4, "tp": other % 4}, device_id_type=MESH,
        )
        copy.start()

    rows = row_own[...]
    for d in range(1, vp_size):
        row_copies[d - 1].wait_recv()
        rows = rows + row_in[d - 1]
    rows_ref[...] = rows
    for copy in row_copies:
        copy.wait_send()
    wait_sends(st.at[pl.ds(0, 3)], st_ssem.at[0])
    wait_sends(give, give_sem.at[0])
    wait_sends(push, push_sem.at[0])
    wait_arrivals(fs.at[pl.ds(0, n_dev - 1)], fs_rsem.at[0])
    wait_sends(fs.at[pl.ds(0, n_dev - 1)], fs_ssem.at[0])
    sums_ref[...] = fs[...]


def tail_kernel(
    n_dev, full_width, z_ref, sums_ref, rows_ref, affine_ref, out_hbm, ls_hbm, nxt_hbm, out, ls, nxt, sem
):
    packed = [sums_ref[i] for i in range(n_dev)]
    n_rows, block = out.shape
    wide = lambda p, i: jnp.broadcast_to(unpack_lanes(p, i, 4), (n_rows, LANES))
    tops = [wide(p, 0) for p in packed]
    all_top = functools.reduce(jnp.maximum, tops)
    all_sum = functools.reduce(jnp.add, [wide(p, 1) * jnp.exp(m - all_top) for p, m in zip(packed, tops)])
    wide_log_sum = all_top + jnp.log(all_sum)
    part = block // OUT_PARTS
    for i in range(OUT_PARTS):
        for k in range(part // LANES):
            tile = pl.ds(i * part + k * LANES, LANES)
            out[:, tile] = z_ref[:, tile] - wide_log_sum
        columns = pl.ds(i * part, part)
        pltpu.make_async_copy(out.at[:, columns], out_hbm.at[:, columns], sem.at[0]).start()
    log_sum = wide_log_sum[:, 0:1]
    square = (n_rows, n_rows)
    on_diag = lax.broadcasted_iota(jnp.int32, square, 0) == lax.broadcasted_iota(jnp.int32, square, 1)
    ls[...] = jnp.sum(jnp.where(on_diag, jnp.broadcast_to(log_sum, square), 0.0), axis=0, keepdims=True)
    ls_copy = pltpu.make_async_copy(ls, ls_hbm, sem.at[1])
    ls_copy.start()
    sums = functools.reduce(jnp.add, [unpack_lanes(p, 2, 4) for p in packed])
    squares = functools.reduce(jnp.add, [unpack_lanes(p, 3, 4) for p in packed])
    nxt[...] = apply_norm(rows_ref[...], sums, squares, affine_ref[0:1, :], affine_ref[1:2, :], full_width)
    nxt_copy = pltpu.make_async_copy(nxt, nxt_hbm, sem.at[2])
    nxt_copy.start()
    pltpu.make_async_copy(out, out_hbm, sem.at[0]).wait()
    ls_copy.wait()
    nxt_copy.wait()


def solution(mesh):
    tp_size = mesh.shape["tp"]
    vp_size = mesh.shape["vp"]
    n_dev = tp_size * vp_size

    def per_device(hidden, lnf_gain, lnf_bias, emb_table, next_tok, eln_gain, eln_bias):
        n_rows, width = hidden.shape
        full_width = width * tp_size
        block = emb_table.shape[0] // tp_size
        sizes = SMALL + (CHUNK,) * ((block - sum(SMALL)) // CHUNK)
        assert sum(sizes) == block
        shared = len(sizes) - 3

        dma = pltpu.SemaphoreType.DMA
        f32 = jnp.float32
        hbm = pl.BlockSpec(memory_space=pltpu.HBM)
        vmem = pl.BlockSpec(memory_space=pltpu.VMEM)
        row = lambda a: a.reshape(1, a.shape[0])
        z, sums, rows, affine = pl.pallas_call(
            functools.partial(main_kernel, vp_size, sizes, shared, full_width),
            out_shape=(
                pltpu.VMEM((n_rows, block), f32),
                pltpu.VMEM((n_dev, SUBLANES, LANES), f32),
                pltpu.VMEM((n_rows, width), f32),
                pltpu.VMEM((2, width), f32),
            ),
            in_specs=[hbm] * 7,
            out_specs=(vmem,) * 4,
            scratch_shapes=[
                pltpu.VMEM((n_rows, width), jnp.bfloat16),
                pltpu.VMEM((1, width), f32),
                pltpu.VMEM((1, width), f32),
                pltpu.VMEM((1, n_rows), jnp.int32),
                pltpu.VMEM((SLOTS, 2, CHUNK, width), jnp.bfloat16),
                pltpu.VMEM((n_rows, width), jnp.bfloat16),
                pltpu.VMEM((n_rows, block), f32),
                pltpu.VMEM((2, n_rows, block), f32),
                pltpu.VMEM((2, n_rows, block), f32),
                pltpu.VMEM((n_rows, block), f32),
                pltpu.VMEM((n_rows, SMALL[0]), f32),
                pltpu.VMEM((tp_size, SUBLANES, LANES), f32),
                pltpu.VMEM((n_rows, width), f32),
                pltpu.VMEM((vp_size - 1, n_rows, width), f32),
                pltpu.VMEM((n_dev, SUBLANES, LANES), f32),
                dma((6,)),
                dma((SLOTS, 2)),
                dma((1,)),
                dma((TAKES,)),
                dma((1,)),
                dma((len(sizes) - shared + 1,)),
                dma((1,)),
                dma((1,)),
                dma((1,)),
                dma((vp_size - 1,)),
                dma((vp_size - 1,)),
                dma((1,)),
                dma((1,)),
            ],
            compiler_params=pltpu.CompilerParams(
                collective_id=0, has_side_effects=True, vmem_limit_bytes=40 * 2**20
            ),
        )(*(
            pltpu.with_memory_space_constraint(a, pltpu.HBM)
            for a in (hidden, row(lnf_gain), row(lnf_bias), emb_table, row(next_tok), row(eln_gain), row(eln_bias))
        ))
        logprobs, log_sum, next_in = pl.pallas_call(
            functools.partial(tail_kernel, n_dev, full_width),
            out_shape=(
                jax.ShapeDtypeStruct((n_rows, block), f32),
                jax.ShapeDtypeStruct((1, n_rows), f32),
                jax.ShapeDtypeStruct((n_rows, width), jnp.bfloat16),
            ),
            in_specs=[vmem] * 4,
            out_specs=(pl.BlockSpec(memory_space=pl.ANY),) * 3,
            scratch_shapes=[
                pltpu.VMEM((n_rows, block), f32),
                pltpu.VMEM((1, n_rows), f32),
                pltpu.VMEM((n_rows, width), jnp.bfloat16),
                dma((3,)),
            ],
            compiler_params=pltpu.CompilerParams(vmem_limit_bytes=12 * 2**20),
        )(*(pltpu.with_memory_space_constraint(a, pltpu.VMEM) for a in (z, sums, rows, affine)))
        return logprobs, log_sum.reshape(n_rows), next_in

    return jax.shard_map(
        per_device,
        mesh=mesh,
        in_specs=(P("dp", "tp"), P("tp"), P("tp"), P("vp", "tp"), P("dp"), P("tp"), P("tp")),
        out_specs=(P("dp", ("vp", "tp")), P("dp"), P("dp", "tp")),
        check_vma=False,
    )
```

```python
import functools

import jax
import jax.numpy as jnp
from jax import lax
from jax.experimental import pallas as pl
from jax.experimental.pallas import tpu as pltpu
from jax.sharding import PartitionSpec as P

NORM_EPS = 1e-5
MESH = pl.DeviceIdType.MESH
LANES = 128
SUBLANES = 8
CHUNK = 1792
SMALL = (640, 1024, 1024)
SLOTS = 4
TAKES = 4
OUT_PARTS = 35


def row_sums(rows_f32):
    return jnp.sum(rows_f32, axis=1, keepdims=True), jnp.sum(rows_f32 * rows_f32, axis=1, keepdims=True)


def pack_lanes(columns):
    halves = [c[i * SUBLANES : (i + 1) * SUBLANES] for c in columns for i in range(2)]
    shape = (SUBLANES, LANES)
    lane = lax.broadcasted_iota(jnp.int32, shape, 1)
    span = LANES // len(halves)
    packed = jnp.broadcast_to(halves[0], shape)
    for i, column in enumerate(halves[1:], 1):
        packed = jnp.where(lane >= i * span, jnp.broadcast_to(column, shape), packed)
    return packed


def unpack_lanes(packed, i, n_columns):
    span = LANES // (2 * n_columns)
    at = 2 * i * span
    return jnp.concatenate([packed[:, at : at + 1], packed[:, at + span : at + span + 1]], axis=0)


def apply_norm(rows_f32, sums, squares, gain, bias, full_width):
    mean = sums / full_width
    var = squares / full_width - mean * mean
    scaled = (rows_f32 - mean) * lax.rsqrt(var + NORM_EPS)
    return (scaled * gain + bias).astype(jnp.bfloat16)


def main_kernel(
    vp_size, sizes, shared, full_width,
    hid_hbm, g1_hbm, b1_hbm, table_ref, tok_hbm, g2_hbm, b2_hbm,
    z_ref, sums_ref, rows_ref, affine_ref,
    hid_ref, g1_ref, b1_ref, tok_ref, tab, xn, push, give, take, land, land_diag, st, row_own, row_in, fs,
    in_sem, tab_sem, give_sem, take_sem, push_sem, land_sem, diag_sem,
    st_ssem, st_rsem, row_ssem, row_rsem, fs_ssem, fs_rsem,
):
    v = lax.axis_index("vp")
    t = lax.axis_index("tp")
    n_dev = vp_size * 4
    me = v * 4 + t
    core = t % 2
    chip = t // 2
    sib = chip * 2 + 1 - core
    across = (1 - chip) * 2 + core
    diag = (1 - chip) * 2 + 1 - core
    n_rows, block = z_ref.shape
    n_small = len(SMALL)
    n_steps = len(sizes)

    hid_copy = pltpu.make_async_copy(hid_hbm, hid_ref, in_sem.at[0])
    hid_copy.start()
    barrier = pltpu.get_barrier_semaphore()
    for d in range(1, n_dev):
        other = (me + d) % n_dev
        pl.semaphore_signal(barrier, inc=1, device_id={"vp": other // 4, "tp": other % 4}, device_id_type=MESH)

    def wait_sends(ref, sem):
        pltpu.make_async_remote_copy(
            ref, ref, sem, st_rsem.at[0], device_id={"tp": sib}, device_id_type=MESH
        ).wait_send()

    def wait_arrivals(ref, sem):
        pltpu.make_async_remote_copy(
            ref, ref, st_ssem.at[0], sem, device_id={"tp": sib}, device_id_type=MESH
        ).wait_recv()

    small = [
        pltpu.make_async_copy(src, dst, in_sem.at[i + 1])
        for i, (src, dst) in enumerate((
            (g1_hbm, g1_ref), (b1_hbm, b1_ref), (tok_hbm, tok_ref),
            (g2_hbm, affine_ref.at[pl.ds(0, 1)]), (b2_hbm, affine_ref.at[pl.ds(1, 1)]),
        ))
    ]
    for copy in small:
        copy.start()

    def columns(step):
        if isinstance(step, int):
            return pl.ds(sum(sizes[:step]), sizes[step])
        return pl.ds(pl.multiple_of(sum(sizes[:n_small]) + (step - n_small) * CHUNK, LANES), CHUNK)

    def table_rows(phase, step, part):
        owner_chip = (1 - chip) if phase == 0 else chip
        owner_core = (1 - core) if part == 0 else core
        where = columns(step)
        return pl.ds(pl.multiple_of((owner_chip * 2 + owner_core) * block + where.start, LANES), where.size)

    def table_copy(phase, step, part):
        slot = (phase * n_steps + step) % SLOTS
        where = table_rows(phase, step, part)
        return pltpu.make_async_copy(
            table_ref.at[where, :], tab.at[slot, part, pl.ds(0, where.size)], tab_sem.at[slot, part]
        )

    def prefetch(phase, step):
        for part in range(2):
            table_copy(phase, step, part).start()

    hid_copy.wait()
    for s in range(SLOTS):
        prefetch(0, s)
    hid = hid_ref[...].astype(jnp.float32)
    st[t] = pack_lanes(row_sums(hid))
    pl.semaphore_wait(barrier, n_dev - 1)

    for target in (across, diag, sib):
        copy = pltpu.make_async_remote_copy(
            st.at[t], st.at[t], st_ssem.at[0], st_rsem.at[0], device_id={"tp": target}, device_id_type=MESH
        )
        copy.start()

    for copy in small:
        copy.wait()
    square = (n_rows, n_rows)
    on_diag = lax.broadcasted_iota(jnp.int32, square, 0) == lax.broadcasted_iota(jnp.int32, square, 1)
    tok_f32 = jnp.broadcast_to(tok_ref[...].astype(jnp.float32), square)
    tok_col = jnp.sum(jnp.where(on_diag, tok_f32, 0.0), axis=1, keepdims=True).astype(jnp.int32)
    tok_col = tok_col - v * (4 * block)
    row_own[...] = jnp.zeros_like(row_own)

    wait_arrivals(st.at[pl.ds(0, 3)], st_rsem.at[0])
    total = st[0] + st[1] + st[2] + st[3]
    wide = lambda i: jnp.broadcast_to(unpack_lanes(total, i, 2), hid.shape)
    xn[...] = apply_norm(hid, wide(0), wide(1), g1_ref[...], b1_ref[...], full_width)

    def give_copy(phase, step):
        where = columns(step)
        return pltpu.make_async_remote_copy(
            give.at[phase, :, where], take.at[phase, :, where], give_sem.at[0],
            take_sem.at[(phase * n_steps + step) % TAKES], device_id={"tp": sib}, device_id_type=MESH,
        )

    def push_copy(step, sem):
        where = columns(step)
        return pltpu.make_async_remote_copy(
            push.at[:, where], land.at[:, where], push_sem.at[0], land_sem.at[sem],
            device_id={"tp": across}, device_id_type=MESH,
        )

    def diag_copy():
        return pltpu.make_async_remote_copy(
            give.at[0, :, columns(0)], land_diag, give_sem.at[0], diag_sem.at[0],
            device_id={"tp": diag}, device_id_type=MESH,
        )

    def combine(phase, step, sem=None, send=True):
        where = columns(step)
        give_copy(phase, step).wait_recv()
        own = push if phase == 0 else z_ref
        own[:, where] = own[:, where] + take[phase, :, where]
        if phase == 0 and send:
            push_copy(step, sem).start()

    def produce(phase, step, select=True):
        where = columns(step)
        slot = (phase * n_steps + step) % SLOTS
        for part in range(2):
            table_copy(phase, step, part).wait()
            vals = lax.dot_general(
                xn[...], tab[slot, part, 0 : where.size, :], (((1,), (1,)), ((), ())), preferred_element_type=jnp.float32
            )
            if part == 0:
                give[phase, :, where] = vals
            elif phase == 0:
                push[:, where] = vals
            else:
                z_ref[:, where] = vals
            if select:
                select_part(phase, step, part)
            if part == 0 and phase == 0 and isinstance(step, int) and step == 0:
                diag_copy().start()
            elif part == 0:
                give_copy(phase, step).start()

    def select_part(phase, step, part):
        where = table_rows(phase, step, part)
        slot = (phase * n_steps + step) % SLOTS
        hit = lax.broadcasted_iota(jnp.int32, (n_rows, where.size), 1) == tok_col - where.start
        ones = jnp.where(hit, 1.0, 0.0).astype(jnp.bfloat16)
        row_own[...] = row_own[...] + jnp.dot(
            ones, tab[slot, part, 0 : where.size, :], preferred_element_type=jnp.float32
        )

    produce(0, 0, select=False)
    push_copy(0, 0).start()
    produce(0, 1, select=False)
    produce(0, 2, select=False)

    def early_rows():
        for step in range(3):
            for part in range(2):
                select_part(0, step, part)

    pl.when(core == 1)(early_rows)
    combine(0, 1, 1)
    pl.when(core == 0)(early_rows)
    for step in range(3):
        prefetch(0, SLOTS + step)

    def far_step(step, carry):
        produce(0, step)
        combine(0, step - 1, 1, send=False)
        hold = (core == 1) & (step >= 4) & (step < 6)

        @pl.when(jnp.logical_not(hold))
        def _():
            push_copy(step - 1, 1).start()

        @pl.when((core == 1) & (step == 6))
        def _():
            push_copy(step - 3, 1).start()
            push_copy(step - 2, 1).start()
        prefetch(0, step + SLOTS)
        return carry

    far_step(n_small, 0)
    lax.fori_loop(n_small + 1, n_steps - SLOTS, far_step, 0)
    for step in range(n_steps - SLOTS, n_steps):
        produce(0, step)
        combine(0, step - 1, max(step - 1 - shared, 0) + 1)
        prefetch(1, step + SLOTS - n_steps)

    for step in range(n_small + 1):
        produce(1, step)
        combine(0, n_steps - 1, n_steps - shared) if step == 0 else combine(1, step - 1)
        prefetch(1, SLOTS + step)

    def near_step(step, carry):
        produce(1, step)
        combine(1, step - 1)

        @pl.when(step + SLOTS < n_steps)
        def _():
            prefetch(1, step + SLOTS)

        return carry

    lax.fori_loop(n_small + 1, n_steps, near_step, 0)

    row_copies = []
    for d in range(1, vp_size):
        copy = pltpu.make_async_remote_copy(
            row_own, row_in.at[d - 1], row_ssem.at[d - 1], row_rsem.at[d - 1],
            device_id={"vp": (v + d) % vp_size}, device_id_type=MESH,
        )
        copy.start()
        row_copies.append(copy)
    combine(1, n_steps - 1)
    own_sums, own_squares = row_sums(row_own[...])

    def finish(step, carry, own_sem=False):
        where = columns(step)
        top, acc = carry
        if own_sem:
            push_copy(step, step - shared + 1).wait_recv()
        vals = z_ref[:, where] + land[:, where]
        if isinstance(step, int) and step == 0:
            vals = vals + land_diag[...]
        z_ref[:, where] = vals
        tiles = [vals[:, i * LANES : (i + 1) * LANES] for i in range(where.size // LANES)]
        new_top = functools.reduce(jnp.maximum, tiles, top)
        acc = acc * jnp.exp(top - new_top)
        for tile in tiles:
            acc = acc + jnp.exp(tile - new_top)
        return new_top, acc

    state = (jnp.full((n_rows, LANES), -jnp.inf, jnp.float32), jnp.zeros((n_rows, LANES), jnp.float32))
    push_copy(0, 0).wait_recv()
    diag_copy().wait_recv()
    together = land.at[:, pl.ds(sizes[0], sum(sizes[1 : shared + 1]))]
    wait_arrivals(together, land_sem.at[1])
    for step in range(n_small):
        state = finish(step, state)
    state = lax.fori_loop(n_small, shared + 1, finish, state)
    top, acc = lax.fori_loop(shared + 1, n_steps, functools.partial(finish, own_sem=True), state)
    row_top = jnp.max(top, axis=1, keepdims=True)
    row_sum = jnp.sum(acc * jnp.exp(top - row_top), axis=1, keepdims=True)
    fs[me] = pack_lanes((row_top, row_sum, own_sums, own_squares))
    for d in range(1, n_dev):
        other = (me + d) % n_dev
        copy = pltpu.make_async_remote_copy(
            fs.at[me], fs.at[me], fs_ssem.at[0], fs_rsem.at[0],
            device_id={"vp": other // 4, "tp": other % 4}, device_id_type=MESH,
        )
        copy.start()

    rows = row_own[...]
    for d in range(1, vp_size):
        row_copies[d - 1].wait_recv()
        rows = rows + row_in[d - 1]
    rows_ref[...] = rows
    for copy in row_copies:
        copy.wait_send()
    wait_sends(st.at[pl.ds(0, 3)], st_ssem.at[0])
    wait_sends(give, give_sem.at[0])
    wait_sends(push, push_sem.at[0])
    wait_arrivals(fs.at[pl.ds(0, n_dev - 1)], fs_rsem.at[0])
    wait_sends(fs.at[pl.ds(0, n_dev - 1)], fs_ssem.at[0])
    sums_ref[...] = fs[...]


def tail_kernel(
    n_dev, full_width, z_ref, sums_ref, rows_ref, affine_ref, out_hbm, ls_hbm, nxt_hbm, out, ls, nxt, sem
):
    packed = [sums_ref[i] for i in range(n_dev)]
    n_rows, block = out.shape
    wide = lambda p, i: jnp.broadcast_to(unpack_lanes(p, i, 4), (n_rows, LANES))
    tops = [wide(p, 0) for p in packed]
    all_top = functools.reduce(jnp.maximum, tops)
    all_sum = functools.reduce(jnp.add, [wide(p, 1) * jnp.exp(m - all_top) for p, m in zip(packed, tops)])
    wide_log_sum = all_top + jnp.log(all_sum)
    part = block // OUT_PARTS
    for i in range(OUT_PARTS):
        for k in range(part // LANES):
            tile = pl.ds(i * part + k * LANES, LANES)
            out[:, tile] = z_ref[:, tile] - wide_log_sum
        columns = pl.ds(i * part, part)
        pltpu.make_async_copy(out.at[:, columns], out_hbm.at[:, columns], sem.at[0]).start()
    log_sum = wide_log_sum[:, 0:1]
    square = (n_rows, n_rows)
    on_diag = lax.broadcasted_iota(jnp.int32, square, 0) == lax.broadcasted_iota(jnp.int32, square, 1)
    ls[...] = jnp.sum(jnp.where(on_diag, jnp.broadcast_to(log_sum, square), 0.0), axis=0, keepdims=True)
    ls_copy = pltpu.make_async_copy(ls, ls_hbm, sem.at[1])
    ls_copy.start()
    sums = functools.reduce(jnp.add, [unpack_lanes(p, 2, 4) for p in packed])
    squares = functools.reduce(jnp.add, [unpack_lanes(p, 3, 4) for p in packed])
    nxt[...] = apply_norm(rows_ref[...], sums, squares, affine_ref[0:1, :], affine_ref[1:2, :], full_width)
    nxt_copy = pltpu.make_async_copy(nxt, nxt_hbm, sem.at[2])
    nxt_copy.start()
    pltpu.make_async_copy(out, out_hbm, sem.at[0]).wait()
    ls_copy.wait()
    nxt_copy.wait()


def solution(mesh):
    tp_size = mesh.shape["tp"]
    vp_size = mesh.shape["vp"]
    n_dev = tp_size * vp_size

    def per_device(hidden, lnf_gain, lnf_bias, emb_table, next_tok, eln_gain, eln_bias):
        n_rows, width = hidden.shape
        full_width = width * tp_size
        block = emb_table.shape[0] // tp_size
        sizes = SMALL + (CHUNK,) * ((block - sum(SMALL)) // CHUNK)
        assert sum(sizes) == block
        shared = len(sizes) - 3

        dma = pltpu.SemaphoreType.DMA
        f32 = jnp.float32
        hbm = pl.BlockSpec(memory_space=pltpu.HBM)
        vmem = pl.BlockSpec(memory_space=pltpu.VMEM)
        row = lambda a: a.reshape(1, a.shape[0])
        z, sums, rows, affine = pl.pallas_call(
            functools.partial(main_kernel, vp_size, sizes, shared, full_width),
            out_shape=(
                pltpu.VMEM((n_rows, block), f32),
                pltpu.VMEM((n_dev, SUBLANES, LANES), f32),
                pltpu.VMEM((n_rows, width), f32),
                pltpu.VMEM((2, width), f32),
            ),
            in_specs=[hbm] * 7,
            out_specs=(vmem,) * 4,
            scratch_shapes=[
                pltpu.VMEM((n_rows, width), jnp.bfloat16),
                pltpu.VMEM((1, width), f32),
                pltpu.VMEM((1, width), f32),
                pltpu.VMEM((1, n_rows), jnp.int32),
                pltpu.VMEM((SLOTS, 2, CHUNK, width), jnp.bfloat16),
                pltpu.VMEM((n_rows, width), jnp.bfloat16),
                pltpu.VMEM((n_rows, block), f32),
                pltpu.VMEM((2, n_rows, block), f32),
                pltpu.VMEM((2, n_rows, block), f32),
                pltpu.VMEM((n_rows, block), f32),
                pltpu.VMEM((n_rows, SMALL[0]), f32),
                pltpu.VMEM((tp_size, SUBLANES, LANES), f32),
                pltpu.VMEM((n_rows, width), f32),
                pltpu.VMEM((vp_size - 1, n_rows, width), f32),
                pltpu.VMEM((n_dev, SUBLANES, LANES), f32),
                dma((6,)),
                dma((SLOTS, 2)),
                dma((1,)),
                dma((TAKES,)),
                dma((1,)),
                dma((len(sizes) - shared + 1,)),
                dma((1,)),
                dma((1,)),
                dma((1,)),
                dma((vp_size - 1,)),
                dma((vp_size - 1,)),
                dma((1,)),
                dma((1,)),
            ],
            compiler_params=pltpu.CompilerParams(
                collective_id=0, has_side_effects=True, vmem_limit_bytes=40 * 2**20
            ),
        )(*(
            pltpu.with_memory_space_constraint(a, pltpu.HBM)
            for a in (hidden, row(lnf_gain), row(lnf_bias), emb_table, row(next_tok), row(eln_gain), row(eln_bias))
        ))
        logprobs, log_sum, next_in = pl.pallas_call(
            functools.partial(tail_kernel, n_dev, full_width),
            out_shape=(
                jax.ShapeDtypeStruct((n_rows, block), f32),
                jax.ShapeDtypeStruct((1, n_rows), f32),
                jax.ShapeDtypeStruct((n_rows, width), jnp.bfloat16),
            ),
            in_specs=[vmem] * 4,
            out_specs=(pl.BlockSpec(memory_space=pl.ANY),) * 3,
            scratch_shapes=[
                pltpu.VMEM((n_rows, block), f32),
                pltpu.VMEM((1, n_rows), f32),
                pltpu.VMEM((n_rows, width), jnp.bfloat16),
                dma((3,)),
            ],
            compiler_params=pltpu.CompilerParams(vmem_limit_bytes=12 * 2**20),
        )(*(pltpu.with_memory_space_constraint(a, pltpu.VMEM) for a in (z, sums, rows, affine)))
        return logprobs, log_sum.reshape(n_rows), next_in

    return jax.shard_map(
        per_device,
        mesh=mesh,
        in_specs=(P("dp", "tp"), P("tp"), P("tp"), P("vp", "tp"), P("dp"), P("tp"), P("tp")),
        out_specs=(P("dp", ("vp", "tp")), P("dp"), P("dp", "tp")),
        check_vma=False,
    )
```

```python
import functools

import jax
import jax.numpy as jnp
from jax import lax
from jax.experimental import pallas as pl
from jax.experimental.pallas import tpu as pltpu
from jax.sharding import PartitionSpec as P

NORM_EPS = 1e-5
MESH = pl.DeviceIdType.MESH
LANES = 128
SUBLANES = 8
CHUNK = 1792
SMALL = (512, 512, 1664)
SLOTS = 4
TAKES = 4
OUT_PARTS = 35


def row_sums(rows_f32):
    return jnp.sum(rows_f32, axis=1, keepdims=True), jnp.sum(rows_f32 * rows_f32, axis=1, keepdims=True)


def pack_lanes(columns):
    halves = [c[i * SUBLANES : (i + 1) * SUBLANES] for c in columns for i in range(2)]
    shape = (SUBLANES, LANES)
    lane = lax.broadcasted_iota(jnp.int32, shape, 1)
    span = LANES // len(halves)
    packed = jnp.broadcast_to(halves[0], shape)
    for i, column in enumerate(halves[1:], 1):
        packed = jnp.where(lane >= i * span, jnp.broadcast_to(column, shape), packed)
    return packed


def unpack_lanes(packed, i, n_columns):
    span = LANES // (2 * n_columns)
    at = 2 * i * span
    return jnp.concatenate([packed[:, at : at + 1], packed[:, at + span : at + span + 1]], axis=0)


def apply_norm(rows_f32, sums, squares, gain, bias, full_width):
    mean = sums / full_width
    var = squares / full_width - mean * mean
    scaled = (rows_f32 - mean) * lax.rsqrt(var + NORM_EPS)
    return (scaled * gain + bias).astype(jnp.bfloat16)


def main_kernel(
    vp_size, sizes, shared, full_width,
    hid_hbm, g1_hbm, b1_hbm, table_ref, tok_hbm, g2_hbm, b2_hbm,
    z_ref, sums_ref, rows_ref, affine_ref,
    hid_ref, g1_ref, b1_ref, tok_ref, tab, xn, push, give, take, land, land_diag, st, row_own, row_in, fs,
    in_sem, tab_sem, give_sem, take_sem, push_sem, land_sem, diag_sem,
    st_ssem, st_rsem, row_ssem, row_rsem, fs_ssem, fs_rsem,
):
    v = lax.axis_index("vp")
    t = lax.axis_index("tp")
    n_dev = vp_size * 4
    me = v * 4 + t
    core = t % 2
    chip = t // 2
    sib = chip * 2 + 1 - core
    across = (1 - chip) * 2 + core
    diag = (1 - chip) * 2 + 1 - core
    n_rows, block = z_ref.shape
    n_small = len(SMALL)
    n_steps = len(sizes)

    hid_copy = pltpu.make_async_copy(hid_hbm, hid_ref, in_sem.at[0])
    hid_copy.start()
    barrier = pltpu.get_barrier_semaphore()
    for d in range(1, n_dev):
        other = (me + d) % n_dev
        pl.semaphore_signal(barrier, inc=1, device_id={"vp": other // 4, "tp": other % 4}, device_id_type=MESH)

    def wait_sends(ref, sem):
        pltpu.make_async_remote_copy(
            ref, ref, sem, st_rsem.at[0], device_id={"tp": sib}, device_id_type=MESH
        ).wait_send()

    def wait_arrivals(ref, sem):
        pltpu.make_async_remote_copy(
            ref, ref, st_ssem.at[0], sem, device_id={"tp": sib}, device_id_type=MESH
        ).wait_recv()

    small = [
        pltpu.make_async_copy(src, dst, in_sem.at[i + 1])
        for i, (src, dst) in enumerate((
            (g1_hbm, g1_ref), (b1_hbm, b1_ref), (tok_hbm, tok_ref),
            (g2_hbm, affine_ref.at[pl.ds(0, 1)]), (b2_hbm, affine_ref.at[pl.ds(1, 1)]),
        ))
    ]
    for copy in small:
        copy.start()

    def columns(step):
        if isinstance(step, int):
            return pl.ds(sum(sizes[:step]), sizes[step])
        return pl.ds(pl.multiple_of(sum(sizes[:n_small]) + (step - n_small) * CHUNK, LANES), CHUNK)

    def table_rows(phase, step, part):
        owner_chip = (1 - chip) if phase == 0 else chip
        owner_core = (1 - core) if part == 0 else core
        where = columns(step)
        return pl.ds(pl.multiple_of((owner_chip * 2 + owner_core) * block + where.start, LANES), where.size)

    def table_copy(phase, step, part):
        slot = (phase * n_steps + step) % SLOTS
        where = table_rows(phase, step, part)
        return pltpu.make_async_copy(
            table_ref.at[where, :], tab.at[slot, part, pl.ds(0, where.size)], tab_sem.at[slot, part]
        )

    def prefetch(phase, step):
        for part in range(2):
            table_copy(phase, step, part).start()

    hid_copy.wait()
    for s in range(SLOTS):
        prefetch(0, s)
    hid = hid_ref[...].astype(jnp.float32)
    st[t] = pack_lanes(row_sums(hid))
    pl.semaphore_wait(barrier, n_dev - 1)

    for target in (across, diag, sib):
        copy = pltpu.make_async_remote_copy(
            st.at[t], st.at[t], st_ssem.at[0], st_rsem.at[0], device_id={"tp": target}, device_id_type=MESH
        )
        copy.start()

    for copy in small:
        copy.wait()
    square = (n_rows, n_rows)
    on_diag = lax.broadcasted_iota(jnp.int32, square, 0) == lax.broadcasted_iota(jnp.int32, square, 1)
    tok_f32 = jnp.broadcast_to(tok_ref[...].astype(jnp.float32), square)
    tok_col = jnp.sum(jnp.where(on_diag, tok_f32, 0.0), axis=1, keepdims=True).astype(jnp.int32)
    tok_col = tok_col - v * (4 * block)
    row_own[...] = jnp.zeros_like(row_own)

    wait_arrivals(st.at[pl.ds(0, 3)], st_rsem.at[0])
    total = st[0] + st[1] + st[2] + st[3]
    wide = lambda i: jnp.broadcast_to(unpack_lanes(total, i, 2), hid.shape)
    xn[...] = apply_norm(hid, wide(0), wide(1), g1_ref[...], b1_ref[...], full_width)

    def give_copy(phase, step):
        where = columns(step)
        return pltpu.make_async_remote_copy(
            give.at[phase, :, where], take.at[phase, :, where], give_sem.at[0],
            take_sem.at[(phase * n_steps + step) % TAKES], device_id={"tp": sib}, device_id_type=MESH,
        )

    def push_copy(step, sem):
        where = columns(step)
        return pltpu.make_async_remote_copy(
            push.at[:, where], land.at[:, where], push_sem.at[0], land_sem.at[sem],
            device_id={"tp": across}, device_id_type=MESH,
        )

    def diag_copy():
        return pltpu.make_async_remote_copy(
            give.at[0, :, columns(0)], land_diag, give_sem.at[0], diag_sem.at[0],
            device_id={"tp": diag}, device_id_type=MESH,
        )

    def combine(phase, step, sem=None, send=True):
        where = columns(step)
        give_copy(phase, step).wait_recv()
        own = push if phase == 0 else z_ref
        own[:, where] = own[:, where] + take[phase, :, where]
        if phase == 0 and send:
            push_copy(step, sem).start()

    def logits_part(phase, step, part):
        where = columns(step)
        slot = (phase * n_steps + step) % SLOTS
        table_copy(phase, step, part).wait()
        vals = lax.dot_general(
            xn[...], tab[slot, part, 0 : where.size, :], (((1,), (1,)), ((), ())), preferred_element_type=jnp.float32
        )
        if part == 0:
            give[phase, :, where] = vals
        elif phase == 0:
            push[:, where] = vals
        else:
            z_ref[:, where] = vals

    def produce(phase, step):
        for part in range(2):
            logits_part(phase, step, part)
            select_part(phase, step, part)
            if part == 0:
                give_copy(phase, step).start()

    def select_part(phase, step, part):
        where = table_rows(phase, step, part)
        slot = (phase * n_steps + step) % SLOTS
        hit = lax.broadcasted_iota(jnp.int32, (n_rows, where.size), 1) == tok_col - where.start
        ones = jnp.where(hit, 1.0, 0.0).astype(jnp.bfloat16)
        row_own[...] = row_own[...] + jnp.dot(
            ones, tab[slot, part, 0 : where.size, :], preferred_element_type=jnp.float32
        )

    logits_part(0, 0, 0)
    diag_copy().start()
    logits_part(0, 1, 0)
    give_copy(0, 1).start()
    logits_part(0, 0, 1)
    push_copy(0, 0).start()
    logits_part(0, 1, 1)
    logits_part(0, 2, 0)
    give_copy(0, 2).start()
    logits_part(0, 2, 1)

    def early_rows(steps):
        for step in steps:
            for part in range(2):
                select_part(0, step, part)
            prefetch(0, SLOTS + step)

    @pl.when(core == 0)
    def _():
        combine(0, 1, 1)
        early_rows((0, 1))
        combine(0, 2, 1)
        early_rows((2,))

    @pl.when(core == 1)
    def _():
        early_rows((0, 1))
        combine(0, 1, 1)
        combine(0, 2, 1)
        early_rows((2,))

    produce(0, n_small)
    prefetch(0, SLOTS + n_small)

    def far_step(step, carry):
        produce(0, step)
        combine(0, step - 1, 1, send=False)
        hold = (core == 1) & (step >= 5) & (step < 8)

        @pl.when(jnp.logical_not(hold))
        def _():
            push_copy(step - 1, 1).start()

        @pl.when((core == 1) & (step == 8))
        def _():
            push_copy(step - 4, 1).start()
            push_copy(step - 3, 1).start()
            push_copy(step - 2, 1).start()

        prefetch(0, step + SLOTS)
        return carry

    lax.fori_loop(n_small + 1, n_steps - SLOTS, far_step, 0)
    for step in range(n_steps - SLOTS, n_steps):
        produce(0, step)
        combine(0, step - 1, max(step - 1 - shared, 0) + 1)
        prefetch(1, step + SLOTS - n_steps)

    for step in range(n_small + 1):
        produce(1, step)
        combine(0, n_steps - 1, n_steps - shared) if step == 0 else combine(1, step - 1)
        prefetch(1, SLOTS + step)

    def near_step(step, carry):
        produce(1, step)
        combine(1, step - 1)

        @pl.when(step + SLOTS < n_steps)
        def _():
            prefetch(1, step + SLOTS)

        return carry

    lax.fori_loop(n_small + 1, n_steps, near_step, 0)

    row_copies = []
    for d in range(1, vp_size):
        copy = pltpu.make_async_remote_copy(
            row_own, row_in.at[d - 1], row_ssem.at[d - 1], row_rsem.at[d - 1],
            device_id={"vp": (v + d) % vp_size}, device_id_type=MESH,
        )
        copy.start()
        row_copies.append(copy)
    combine(1, n_steps - 1)
    own_sums, own_squares = row_sums(row_own[...])

    def finish(step, carry, own_sem=False):
        where = columns(step)
        top, acc = carry
        if own_sem:
            push_copy(step, step - shared + 1).wait_recv()
        vals = z_ref[:, where] + land[:, where]
        if isinstance(step, int) and step == 0:
            vals = vals + land_diag[...]
        z_ref[:, where] = vals
        tiles = [vals[:, i * LANES : (i + 1) * LANES] for i in range(where.size // LANES)]
        new_top = functools.reduce(jnp.maximum, tiles, top)
        acc = acc * jnp.exp(top - new_top)
        for tile in tiles:
            acc = acc + jnp.exp(tile - new_top)
        return new_top, acc

    state = (jnp.full((n_rows, LANES), -jnp.inf, jnp.float32), jnp.zeros((n_rows, LANES), jnp.float32))
    push_copy(0, 0).wait_recv()
    diag_copy().wait_recv()
    together = land.at[:, pl.ds(sizes[0], sum(sizes[1 : shared + 1]))]
    wait_arrivals(together, land_sem.at[1])
    for step in range(n_small):
        state = finish(step, state)
    state = lax.fori_loop(n_small, shared + 1, finish, state)
    top, acc = lax.fori_loop(shared + 1, n_steps, functools.partial(finish, own_sem=True), state)
    row_top = jnp.max(top, axis=1, keepdims=True)
    row_sum = jnp.sum(acc * jnp.exp(top - row_top), axis=1, keepdims=True)
    fs[me] = pack_lanes((row_top, row_sum, own_sums, own_squares))
    for d in range(n_dev - 1):
        other = d + (d - me + n_dev) // n_dev
        copy = pltpu.make_async_remote_copy(
            fs.at[me], fs.at[me], fs_ssem.at[0], fs_rsem.at[0],
            device_id={"vp": other // 4, "tp": other % 4}, device_id_type=MESH,
        )
        copy.start()

    rows = row_own[...]
    for d in range(1, vp_size):
        row_copies[d - 1].wait_recv()
        rows = rows + row_in[d - 1]
    rows_ref[...] = rows
    for copy in row_copies:
        copy.wait_send()
    wait_sends(st.at[pl.ds(0, 3)], st_ssem.at[0])
    wait_sends(give, give_sem.at[0])
    wait_sends(push, push_sem.at[0])
    wait_arrivals(fs.at[pl.ds(0, n_dev - 1)], fs_rsem.at[0])
    wait_sends(fs.at[pl.ds(0, n_dev - 1)], fs_ssem.at[0])
    sums_ref[...] = fs[...]


def tail_kernel(
    n_dev, full_width, z_ref, sums_ref, rows_ref, affine_ref, out_hbm, ls_hbm, nxt_hbm, out, ls, nxt, sem
):
    packed = [sums_ref[i] for i in range(n_dev)]
    n_rows, block = out.shape
    wide = lambda p, i: jnp.broadcast_to(unpack_lanes(p, i, 4), (n_rows, LANES))
    tops = [wide(p, 0) for p in packed]
    all_top = functools.reduce(jnp.maximum, tops)
    all_sum = functools.reduce(jnp.add, [wide(p, 1) * jnp.exp(m - all_top) for p, m in zip(packed, tops)])
    wide_log_sum = all_top + jnp.log(all_sum)
    part = block // OUT_PARTS
    for i in range(OUT_PARTS):
        for k in range(part // LANES):
            tile = pl.ds(i * part + k * LANES, LANES)
            out[:, tile] = z_ref[:, tile] - wide_log_sum
        columns = pl.ds(i * part, part)
        pltpu.make_async_copy(out.at[:, columns], out_hbm.at[:, columns], sem.at[0]).start()
    log_sum = wide_log_sum[:, 0:1]
    square = (n_rows, n_rows)
    on_diag = lax.broadcasted_iota(jnp.int32, square, 0) == lax.broadcasted_iota(jnp.int32, square, 1)
    ls[...] = jnp.sum(jnp.where(on_diag, jnp.broadcast_to(log_sum, square), 0.0), axis=0, keepdims=True)
    ls_copy = pltpu.make_async_copy(ls, ls_hbm, sem.at[1])
    ls_copy.start()
    sums = functools.reduce(jnp.add, [unpack_lanes(p, 2, 4) for p in packed])
    squares = functools.reduce(jnp.add, [unpack_lanes(p, 3, 4) for p in packed])
    nxt[...] = apply_norm(rows_ref[...], sums, squares, affine_ref[0:1, :], affine_ref[1:2, :], full_width)
    nxt_copy = pltpu.make_async_copy(nxt, nxt_hbm, sem.at[2])
    nxt_copy.start()
    pltpu.make_async_copy(out, out_hbm, sem.at[0]).wait()
    ls_copy.wait()
    nxt_copy.wait()


def solution(mesh):
    tp_size = mesh.shape["tp"]
    vp_size = mesh.shape["vp"]
    n_dev = tp_size * vp_size

    def per_device(hidden, lnf_gain, lnf_bias, emb_table, next_tok, eln_gain, eln_bias):
        n_rows, width = hidden.shape
        full_width = width * tp_size
        block = emb_table.shape[0] // tp_size
        sizes = SMALL + (CHUNK,) * ((block - sum(SMALL)) // CHUNK)
        assert sum(sizes) == block
        shared = len(sizes) - 3

        dma = pltpu.SemaphoreType.DMA
        f32 = jnp.float32
        hbm = pl.BlockSpec(memory_space=pltpu.HBM)
        vmem = pl.BlockSpec(memory_space=pltpu.VMEM)
        row = lambda a: a.reshape(1, a.shape[0])
        z, sums, rows, affine = pl.pallas_call(
            functools.partial(main_kernel, vp_size, sizes, shared, full_width),
            out_shape=(
                pltpu.VMEM((n_rows, block), f32),
                pltpu.VMEM((n_dev, SUBLANES, LANES), f32),
                pltpu.VMEM((n_rows, width), f32),
                pltpu.VMEM((2, width), f32),
            ),
            in_specs=[hbm] * 7,
            out_specs=(vmem,) * 4,
            scratch_shapes=[
                pltpu.VMEM((n_rows, width), jnp.bfloat16),
                pltpu.VMEM((1, width), f32),
                pltpu.VMEM((1, width), f32),
                pltpu.VMEM((1, n_rows), jnp.int32),
                pltpu.VMEM((SLOTS, 2, CHUNK, width), jnp.bfloat16),
                pltpu.VMEM((n_rows, width), jnp.bfloat16),
                pltpu.VMEM((n_rows, block), f32),
                pltpu.VMEM((2, n_rows, block), f32),
                pltpu.VMEM((2, n_rows, block), f32),
                pltpu.VMEM((n_rows, block), f32),
                pltpu.VMEM((n_rows, SMALL[0]), f32),
                pltpu.VMEM((tp_size, SUBLANES, LANES), f32),
                pltpu.VMEM((n_rows, width), f32),
                pltpu.VMEM((vp_size - 1, n_rows, width), f32),
                pltpu.VMEM((n_dev, SUBLANES, LANES), f32),
                dma((6,)),
                dma((SLOTS, 2)),
                dma((1,)),
                dma((TAKES,)),
                dma((1,)),
                dma((len(sizes) - shared + 1,)),
                dma((1,)),
                dma((1,)),
                dma((1,)),
                dma((vp_size - 1,)),
                dma((vp_size - 1,)),
                dma((1,)),
                dma((1,)),
            ],
            compiler_params=pltpu.CompilerParams(
                collective_id=0, has_side_effects=True, vmem_limit_bytes=40 * 2**20
            ),
        )(*(
            pltpu.with_memory_space_constraint(a, pltpu.HBM)
            for a in (hidden, row(lnf_gain), row(lnf_bias), emb_table, row(next_tok), row(eln_gain), row(eln_bias))
        ))
        logprobs, log_sum, next_in = pl.pallas_call(
            functools.partial(tail_kernel, n_dev, full_width),
            out_shape=(
                jax.ShapeDtypeStruct((n_rows, block), f32),
                jax.ShapeDtypeStruct((1, n_rows), f32),
                jax.ShapeDtypeStruct((n_rows, width), jnp.bfloat16),
            ),
            in_specs=[vmem] * 4,
            out_specs=(pl.BlockSpec(memory_space=pl.ANY),) * 3,
            scratch_shapes=[
                pltpu.VMEM((n_rows, block), f32),
                pltpu.VMEM((1, n_rows), f32),
                pltpu.VMEM((n_rows, width), jnp.bfloat16),
                dma((3,)),
            ],
            compiler_params=pltpu.CompilerParams(vmem_limit_bytes=12 * 2**20),
        )(*(pltpu.with_memory_space_constraint(a, pltpu.VMEM) for a in (z, sums, rows, affine)))
        return logprobs, log_sum.reshape(n_rows), next_in

    return jax.shard_map(
        per_device,
        mesh=mesh,
        in_specs=(P("dp", "tp"), P("tp"), P("tp"), P("vp", "tp"), P("dp"), P("tp"), P("tp")),
        out_specs=(P("dp", ("vp", "tp")), P("dp"), P("dp", "tp")),
        check_vma=False,
    )
```

```python
import functools

import jax
import jax.numpy as jnp
from jax import lax
from jax.experimental import pallas as pl
from jax.experimental.pallas import tpu as pltpu
from jax.sharding import PartitionSpec as P

NORM_EPS = 1e-5
MESH = pl.DeviceIdType.MESH
LANES = 128
SUBLANES = 8
CHUNK = 1792
SMALL = (512, 512, 1664)
SLOTS = 4
TAKES = 4
OUT_PARTS = 35


def row_sums(rows_f32):
    return jnp.sum(rows_f32, axis=1, keepdims=True), jnp.sum(rows_f32 * rows_f32, axis=1, keepdims=True)


def pack_lanes(columns):
    halves = [c[i * SUBLANES : (i + 1) * SUBLANES] for c in columns for i in range(2)]
    shape = (SUBLANES, LANES)
    lane = lax.broadcasted_iota(jnp.int32, shape, 1)
    span = LANES // len(halves)
    packed = jnp.broadcast_to(halves[0], shape)
    for i, column in enumerate(halves[1:], 1):
        packed = jnp.where(lane >= i * span, jnp.broadcast_to(column, shape), packed)
    return packed


def unpack_lanes(packed, i, n_columns):
    span = LANES // (2 * n_columns)
    at = 2 * i * span
    return jnp.concatenate([packed[:, at : at + 1], packed[:, at + span : at + span + 1]], axis=0)


def apply_norm(rows_f32, sums, squares, gain, bias, full_width):
    mean = sums / full_width
    var = squares / full_width - mean * mean
    scaled = (rows_f32 - mean) * lax.rsqrt(var + NORM_EPS)
    return (scaled * gain + bias).astype(jnp.bfloat16)


def main_kernel(
    vp_size, sizes, shared, full_width,
    hid_hbm, g1_hbm, b1_hbm, table_ref, tok_hbm, g2_hbm, b2_hbm,
    z_ref, sums_ref, rows_ref, affine_ref,
    hid_ref, g1_ref, b1_ref, tok_ref, tab, xn, push, give, take, land, land_diag, st, row_own, row_in, fs,
    in_sem, tab_sem, give_sem, take_sem, push_sem, land_sem, diag_sem,
    st_ssem, st_rsem, row_ssem, row_rsem, fs_ssem, fs_rsem,
):
    v = lax.axis_index("vp")
    t = lax.axis_index("tp")
    n_dev = vp_size * 4
    me = v * 4 + t
    core = t % 2
    chip = t // 2
    sib = chip * 2 + 1 - core
    across = (1 - chip) * 2 + core
    diag = (1 - chip) * 2 + 1 - core
    n_rows, block = z_ref.shape
    n_small = len(SMALL)
    n_steps = len(sizes)

    hid_copy = pltpu.make_async_copy(hid_hbm, hid_ref, in_sem.at[0])
    hid_copy.start()
    barrier = pltpu.get_barrier_semaphore()
    for d in range(1, n_dev):
        other = (me + d) % n_dev
        pl.semaphore_signal(barrier, inc=1, device_id={"vp": other // 4, "tp": other % 4}, device_id_type=MESH)

    def wait_sends(ref, sem):
        pltpu.make_async_remote_copy(
            ref, ref, sem, st_rsem.at[0], device_id={"tp": sib}, device_id_type=MESH
        ).wait_send()

    def wait_arrivals(ref, sem):
        pltpu.make_async_remote_copy(
            ref, ref, st_ssem.at[0], sem, device_id={"tp": sib}, device_id_type=MESH
        ).wait_recv()

    small = [
        pltpu.make_async_copy(src, dst, in_sem.at[1])
        for src, dst in (
            (g1_hbm, g1_ref), (b1_hbm, b1_ref), (tok_hbm, tok_ref),
            (g2_hbm, affine_ref.at[pl.ds(0, 1)]), (b2_hbm, affine_ref.at[pl.ds(1, 1)]),
        )
    ]
    for copy in small:
        copy.start()

    def columns(step):
        if isinstance(step, int):
            return pl.ds(sum(sizes[:step]), sizes[step])
        return pl.ds(pl.multiple_of(sum(sizes[:n_small]) + (step - n_small) * CHUNK, LANES), CHUNK)

    def table_rows(phase, step, part):
        owner_chip = (1 - chip) if phase == 0 else chip
        owner_core = (1 - core) if part == 0 else core
        where = columns(step)
        return pl.ds(pl.multiple_of((owner_chip * 2 + owner_core) * block + where.start, LANES), where.size)

    def table_copy(phase, step, part):
        slot = (phase * n_steps + step) % SLOTS
        where = table_rows(phase, step, part)
        return pltpu.make_async_copy(
            table_ref.at[where, :], tab.at[slot, part, pl.ds(0, where.size)], tab_sem.at[slot, part]
        )

    def prefetch(phase, step):
        for part in range(2):
            table_copy(phase, step, part).start()

    hid_copy.wait()
    for s in range(SLOTS):
        prefetch(0, s)
    hid = hid_ref[...].astype(jnp.float32)
    st[t] = pack_lanes(row_sums(hid))
    pl.semaphore_wait(barrier, n_dev - 1)

    for target in (across, diag, sib):
        copy = pltpu.make_async_remote_copy(
            st.at[t], st.at[t], st_ssem.at[0], st_rsem.at[0], device_id={"tp": target}, device_id_type=MESH
        )
        copy.start()

    for copy in small:
        copy.wait()
    square = (n_rows, n_rows)
    on_diag = lax.broadcasted_iota(jnp.int32, square, 0) == lax.broadcasted_iota(jnp.int32, square, 1)
    tok_f32 = jnp.broadcast_to(tok_ref[...].astype(jnp.float32), square)
    tok_col = jnp.sum(jnp.where(on_diag, tok_f32, 0.0), axis=1, keepdims=True).astype(jnp.int32)
    tok_col = tok_col - v * (4 * block)
    row_own[...] = jnp.zeros_like(row_own)

    wait_arrivals(st.at[pl.ds(0, 3)], st_rsem.at[0])
    total = st[0] + st[1] + st[2] + st[3]
    wide = lambda i: jnp.broadcast_to(unpack_lanes(total, i, 2), hid.shape)
    xn[...] = apply_norm(hid, wide(0), wide(1), g1_ref[...], b1_ref[...], full_width)

    def give_copy(phase, step):
        where = columns(step)
        return pltpu.make_async_remote_copy(
            give.at[phase, :, where], take.at[phase, :, where], give_sem.at[0],
            take_sem.at[(phase * n_steps + step) % TAKES], device_id={"tp": sib}, device_id_type=MESH,
        )

    def push_copy(step, sem):
        where = columns(step)
        return pltpu.make_async_remote_copy(
            push.at[:, where], land.at[:, where], push_sem.at[0], land_sem.at[sem],
            device_id={"tp": across}, device_id_type=MESH,
        )

    def diag_copy():
        return pltpu.make_async_remote_copy(
            give.at[0, :, columns(0)], land_diag, give_sem.at[0], diag_sem.at[0],
            device_id={"tp": diag}, device_id_type=MESH,
        )

    def combine(phase, step, sem=None, send=True):
        where = columns(step)
        give_copy(phase, step).wait_recv()
        own = push if phase == 0 else z_ref
        own[:, where] = own[:, where] + take[phase, :, where]
        if phase == 0 and send:
            push_copy(step, sem).start()

    def logits_part(phase, step, part):
        where = columns(step)
        slot = (phase * n_steps + step) % SLOTS
        table_copy(phase, step, part).wait()
        vals = lax.dot_general(
            xn[...], tab[slot, part, 0 : where.size, :], (((1,), (1,)), ((), ())), preferred_element_type=jnp.float32
        )
        if part == 0:
            give[phase, :, where] = vals
        elif phase == 0:
            push[:, where] = vals
        else:
            z_ref[:, where] = vals

    def produce(phase, step):
        for part in range(2):
            logits_part(phase, step, part)
            select_part(phase, step, part)
            if part == 0:
                give_copy(phase, step).start()

    def select_part(phase, step, part):
        where = table_rows(phase, step, part)
        slot = (phase * n_steps + step) % SLOTS
        hit = lax.broadcasted_iota(jnp.int32, (n_rows, where.size), 1) == tok_col - where.start
        ones = jnp.where(hit, 1.0, 0.0).astype(jnp.bfloat16)
        row_own[...] = row_own[...] + jnp.dot(
            ones, tab[slot, part, 0 : where.size, :], preferred_element_type=jnp.float32
        )

    logits_part(0, 0, 0)
    diag_copy().start()
    logits_part(0, 1, 0)
    give_copy(0, 1).start()
    logits_part(0, 0, 1)
    push_copy(0, 0).start()
    logits_part(0, 1, 1)
    logits_part(0, 2, 0)
    give_copy(0, 2).start()
    logits_part(0, 2, 1)

    def early_rows(steps):
        for step in steps:
            for part in range(2):
                select_part(0, step, part)
            prefetch(0, SLOTS + step)

    @pl.when(core == 0)
    def _():
        combine(0, 1, 1)
        early_rows((0, 1))
        combine(0, 2, 1)
        early_rows((2,))

    @pl.when(core == 1)
    def _():
        early_rows((0, 1))
        combine(0, 1, 1)
        combine(0, 2, 1)
        early_rows((2,))

    produce(0, n_small)
    prefetch(0, SLOTS + n_small)

    def far_step(step, carry):
        produce(0, step)
        combine(0, step - 1, 1, send=False)
        hold = (core == 1) & (step >= 5) & (step < 8)

        @pl.when(jnp.logical_not(hold))
        def _():
            push_copy(step - 1, 1).start()

        @pl.when((core == 1) & (step == 8))
        def _():
            push_copy(step - 4, 1).start()
            push_copy(step - 3, 1).start()
            push_copy(step - 2, 1).start()

        prefetch(0, step + SLOTS)
        return carry

    lax.fori_loop(n_small + 1, n_steps - SLOTS, far_step, 0)
    for step in range(n_steps - SLOTS, n_steps):
        produce(0, step)
        combine(0, step - 1, max(step - 1 - shared, 0) + 1)
        prefetch(1, step + SLOTS - n_steps)

    for step in range(n_small + 1):
        produce(1, step)
        combine(0, n_steps - 1, n_steps - shared) if step == 0 else combine(1, step - 1)
        prefetch(1, SLOTS + step)

    def near_step(step, carry):
        produce(1, step)
        combine(1, step - 1)

        @pl.when(step + SLOTS < n_steps)
        def _():
            prefetch(1, step + SLOTS)

        return carry

    lax.fori_loop(n_small + 1, n_steps, near_step, 0)

    row_copies = []
    for d in range(1, vp_size):
        copy = pltpu.make_async_remote_copy(
            row_own, row_in.at[d - 1], row_ssem.at[d - 1], row_rsem.at[d - 1],
            device_id={"vp": (v + d) % vp_size}, device_id_type=MESH,
        )
        copy.start()
        row_copies.append(copy)
    combine(1, n_steps - 1)
    own_sums, own_squares = row_sums(row_own[...])

    def finish(step, carry, own_sem=False):
        where = columns(step)
        top, acc = carry
        if own_sem:
            push_copy(step, step - shared + 1).wait_recv()
        vals = z_ref[:, where] + land[:, where]
        if isinstance(step, int) and step == 0:
            vals = vals + land_diag[...]
        z_ref[:, where] = vals
        tiles = [vals[:, i * LANES : (i + 1) * LANES] for i in range(where.size // LANES)]
        new_top = functools.reduce(jnp.maximum, tiles, top)
        acc = acc * jnp.exp(top - new_top)
        for tile in tiles:
            acc = acc + jnp.exp(tile - new_top)
        return new_top, acc

    state = (jnp.full((n_rows, LANES), -jnp.inf, jnp.float32), jnp.zeros((n_rows, LANES), jnp.float32))
    push_copy(0, 0).wait_recv()
    diag_copy().wait_recv()
    together = land.at[:, pl.ds(sizes[0], sum(sizes[1 : shared + 1]))]
    wait_arrivals(together, land_sem.at[1])
    for step in range(n_small):
        state = finish(step, state)
    state = lax.fori_loop(n_small, shared + 1, finish, state)
    top, acc = lax.fori_loop(shared + 1, n_steps, functools.partial(finish, own_sem=True), state)
    row_top = jnp.max(top, axis=1, keepdims=True)
    row_sum = jnp.sum(acc * jnp.exp(top - row_top), axis=1, keepdims=True)
    fs[me] = pack_lanes((row_top, row_sum, own_sums, own_squares))
    for d in range(n_dev - 1):
        other = d + (d - me + n_dev) // n_dev
        copy = pltpu.make_async_remote_copy(
            fs.at[me], fs.at[me], fs_ssem.at[0], fs_rsem.at[0],
            device_id={"vp": other // 4, "tp": other % 4}, device_id_type=MESH,
        )
        copy.start()

    rows = row_own[...]
    for d in range(1, vp_size):
        row_copies[d - 1].wait_recv()
        rows = rows + row_in[d - 1]
    rows_ref[...] = rows
    for copy in row_copies:
        copy.wait_send()
    wait_sends(st.at[pl.ds(0, 3)], st_ssem.at[0])
    wait_sends(give, give_sem.at[0])
    wait_sends(push, push_sem.at[0])
    wait_arrivals(fs.at[pl.ds(0, n_dev - 1)], fs_rsem.at[0])
    wait_sends(fs.at[pl.ds(0, n_dev - 1)], fs_ssem.at[0])
    sums_ref[...] = fs[...]


def tail_kernel(
    n_dev, full_width, z_ref, sums_ref, rows_ref, affine_ref, out_hbm, ls_hbm, nxt_hbm, out, ls, nxt, sem
):
    packed = [sums_ref[i] for i in range(n_dev)]
    n_rows, block = out.shape
    wide = lambda p, i: jnp.broadcast_to(unpack_lanes(p, i, 4), (n_rows, LANES))
    tops = [wide(p, 0) for p in packed]
    all_top = functools.reduce(jnp.maximum, tops)
    all_sum = functools.reduce(jnp.add, [wide(p, 1) * jnp.exp(m - all_top) for p, m in zip(packed, tops)])
    wide_log_sum = all_top + jnp.log(all_sum)
    part = block // OUT_PARTS
    for i in range(OUT_PARTS):
        for k in range(part // LANES):
            tile = pl.ds(i * part + k * LANES, LANES)
            out[:, tile] = z_ref[:, tile] - wide_log_sum
        columns = pl.ds(i * part, part)
        pltpu.make_async_copy(out.at[:, columns], out_hbm.at[:, columns], sem.at[0]).start()
    log_sum = wide_log_sum[:, 0:1]
    square = (n_rows, n_rows)
    on_diag = lax.broadcasted_iota(jnp.int32, square, 0) == lax.broadcasted_iota(jnp.int32, square, 1)
    ls[...] = jnp.sum(jnp.where(on_diag, jnp.broadcast_to(log_sum, square), 0.0), axis=0, keepdims=True)
    ls_copy = pltpu.make_async_copy(ls, ls_hbm, sem.at[1])
    ls_copy.start()
    sums = functools.reduce(jnp.add, [unpack_lanes(p, 2, 4) for p in packed])
    squares = functools.reduce(jnp.add, [unpack_lanes(p, 3, 4) for p in packed])
    nxt[...] = apply_norm(rows_ref[...], sums, squares, affine_ref[0:1, :], affine_ref[1:2, :], full_width)
    nxt_copy = pltpu.make_async_copy(nxt, nxt_hbm, sem.at[2])
    nxt_copy.start()
    pltpu.make_async_copy(out, out_hbm, sem.at[0]).wait()
    ls_copy.wait()
    nxt_copy.wait()


def solution(mesh):
    tp_size = mesh.shape["tp"]
    vp_size = mesh.shape["vp"]
    n_dev = tp_size * vp_size

    def per_device(hidden, lnf_gain, lnf_bias, emb_table, next_tok, eln_gain, eln_bias):
        n_rows, width = hidden.shape
        full_width = width * tp_size
        block = emb_table.shape[0] // tp_size
        sizes = SMALL + (CHUNK,) * ((block - sum(SMALL)) // CHUNK)
        assert sum(sizes) == block
        shared = len(sizes) - 3

        dma = pltpu.SemaphoreType.DMA
        f32 = jnp.float32
        hbm = pl.BlockSpec(memory_space=pltpu.HBM)
        vmem = pl.BlockSpec(memory_space=pltpu.VMEM)
        row = lambda a: a.reshape(1, a.shape[0])
        z, sums, rows, affine = pl.pallas_call(
            functools.partial(main_kernel, vp_size, sizes, shared, full_width),
            out_shape=(
                pltpu.VMEM((n_rows, block), f32),
                pltpu.VMEM((n_dev, SUBLANES, LANES), f32),
                pltpu.VMEM((n_rows, width), f32),
                pltpu.VMEM((2, width), f32),
            ),
            in_specs=[hbm] * 7,
            out_specs=(vmem,) * 4,
            scratch_shapes=[
                pltpu.VMEM((n_rows, width), jnp.bfloat16),
                pltpu.VMEM((1, width), f32),
                pltpu.VMEM((1, width), f32),
                pltpu.VMEM((1, n_rows), jnp.int32),
                pltpu.VMEM((SLOTS, 2, CHUNK, width), jnp.bfloat16),
                pltpu.VMEM((n_rows, width), jnp.bfloat16),
                pltpu.VMEM((n_rows, block), f32),
                pltpu.VMEM((2, n_rows, block), f32),
                pltpu.VMEM((2, n_rows, block), f32),
                pltpu.VMEM((n_rows, block), f32),
                pltpu.VMEM((n_rows, SMALL[0]), f32),
                pltpu.VMEM((tp_size, SUBLANES, LANES), f32),
                pltpu.VMEM((n_rows, width), f32),
                pltpu.VMEM((vp_size - 1, n_rows, width), f32),
                pltpu.VMEM((n_dev, SUBLANES, LANES), f32),
                dma((2,)),
                dma((SLOTS, 2)),
                dma((1,)),
                dma((TAKES,)),
                dma((1,)),
                dma((len(sizes) - shared + 1,)),
                dma((1,)),
                dma((1,)),
                dma((1,)),
                dma((vp_size - 1,)),
                dma((vp_size - 1,)),
                dma((1,)),
                dma((1,)),
            ],
            compiler_params=pltpu.CompilerParams(
                collective_id=0, has_side_effects=True, vmem_limit_bytes=40 * 2**20
            ),
        )(*(
            pltpu.with_memory_space_constraint(a, pltpu.HBM)
            for a in (hidden, row(lnf_gain), row(lnf_bias), emb_table, row(next_tok), row(eln_gain), row(eln_bias))
        ))
        logprobs, log_sum, next_in = pl.pallas_call(
            functools.partial(tail_kernel, n_dev, full_width),
            out_shape=(
                jax.ShapeDtypeStruct((n_rows, block), f32),
                jax.ShapeDtypeStruct((1, n_rows), f32),
                jax.ShapeDtypeStruct((n_rows, width), jnp.bfloat16),
            ),
            in_specs=[vmem] * 4,
            out_specs=(pl.BlockSpec(memory_space=pl.ANY),) * 3,
            scratch_shapes=[
                pltpu.VMEM((n_rows, block), f32),
                pltpu.VMEM((1, n_rows), f32),
                pltpu.VMEM((n_rows, width), jnp.bfloat16),
                dma((3,)),
            ],
            compiler_params=pltpu.CompilerParams(vmem_limit_bytes=12 * 2**20),
        )(*(pltpu.with_memory_space_constraint(a, pltpu.VMEM) for a in (z, sums, rows, affine)))
        return logprobs, log_sum.reshape(n_rows), next_in

    return jax.shard_map(
        per_device,
        mesh=mesh,
        in_specs=(P("dp", "tp"), P("tp"), P("tp"), P("vp", "tp"), P("dp"), P("tp"), P("tp")),
        out_specs=(P("dp", ("vp", "tp")), P("dp"), P("dp", "tp")),
        check_vma=False,
    )
```
